32 devices in a mesh: dp: 4 (over y, z), dcp: 8 (over x, core).
Axes of the slice: x: 4, y: 2, z: 2, core: 2. Of those that a mesh axis runs over, the one named last changes fastest.
The devices are a block of a 4x4x8 slice.
Arguments:
- q_abs: bfloat16 [128, 128, 576], P('dp', 'dcp'), parts along dimension 0
- cache: bfloat16 [128, 8192, 576], P('dp', 'dcp'), parts along dimension 0
- lengths: int32 [128], P('dp'), parts along dimension 0
Outputs:
- output: bfloat16 [128, 128, 512], P('dp', 'dcp'), parts along dimension 0
There are 4 independent parts. The reference program is written for one: setup_inputs(seed, part) draws one part's arguments, and reference() takes and returns one part's arrays. A program takes and returns all parts, laid end to end along the dimension named above; each array names one.
All inputs are finite; a program needn't handle non-finite values.
Results may differ from the reference program's by a relative error of at most 0.00716151.
Values are sent between devices in bfloat16 or wider.
A program may use at most 768 MiB of HBM per device.

```python
import jax
import jax.numpy as jnp
from jax import lax

HEADS = 128
KV_RANK = 512
ROPE = 64
QK_NOPE = 128
B = 32
S = 8192
NDEV = 8

WIDTH = KV_RANK + ROPE
SCALE = (QK_NOPE + ROPE) ** -0.5
BLOCK = S // NDEV
SEG = S // 32


def setup_inputs(seed: int = 0, part: int = 0) -> dict:
    key = jax.random.fold_in(jax.random.key(seed), part)
    kq, kc, kf, ks = jax.random.split(key, 4)
    q_abs = (jax.random.normal(kq, (B, HEADS, WIDTH), jnp.float32) * 0.6).astype(jnp.bfloat16)

    def draw(k):
        k1, k2, k3 = jax.random.split(k, 3)
        seg = jax.random.normal(k1, (32, KV_RANK), jnp.float32)
        lat = jax.random.normal(k2, (S, KV_RANK), jnp.float32) + jnp.repeat(seg, SEG, axis=0)
        rope = jax.random.normal(k3, (S, ROPE), jnp.float32) * 3.0
        return jnp.concatenate([lat, rope], axis=1).astype(jnp.bfloat16)

    cache = lax.map(draw, jax.random.split(kc, B))
    full = S - jax.random.randint(kf, (B,), 0, S // 64)
    short = jax.random.randint(ks, (B,), 1, S + 1)
    lengths = jnp.where(jnp.arange(B) % 2 == 0, full, short).astype(jnp.int32)
    return {'q_abs': q_abs, 'cache': cache, 'lengths': lengths}


def reference(q_abs, cache, lengths):
    pos = jnp.arange(S).reshape(NDEV, BLOCK)

    def one(args):
        qb, cb, lb = args
        cf = cb.astype(jnp.float32).reshape(NDEV, BLOCK, WIDTH)
        s = jnp.einsum('hk,ntk->nht', qb.astype(jnp.float32), cf) * SCALE
        valid = pos < lb
        s = jnp.where(valid[:, None, :], s, -jnp.inf)
        m = jnp.max(s, axis=2)
        m0 = jnp.where(jnp.isfinite(m), m, 0.0)
        p = jnp.exp(s - m0[:, :, None])
        l = jnp.sum(p, axis=2)
        pb = p.astype(jnp.bfloat16).astype(jnp.float32)
        pv = jnp.einsum('nht,ntc->nhc', pb, cf[:, :, :KV_RANK])
        has = l > 0.0
        l1 = jnp.where(has, l, 1.0)
        od = (pv / l1[:, :, None]).astype(jnp.bfloat16).astype(jnp.float32)
        lse_d = jnp.where(has, m0 + jnp.log(l1), -jnp.inf)
        mx = jnp.max(lse_d, axis=0)
        lse = mx + jnp.log(jnp.sum(jnp.exp(lse_d - mx[None, :]), axis=0))
        o = jnp.sum(jnp.exp(lse_d - lse[None, :])[:, :, None] * od, axis=0)
        return o.astype(jnp.bfloat16)

    return lax.map(one, (q_abs, cache, lengths))
```

```python
import functools

import jax
import jax.numpy as jnp
from jax import lax
from jax.experimental import pallas as pl
from jax.experimental.pallas import tpu as pltpu
from jax.sharding import PartitionSpec as P

ROPE = 64
SCALE = 192 ** -0.5
F32 = jnp.float32
BF16 = jnp.bfloat16
NT = (((1,), (1,)), ((), ()))

SC = 4
H = SC // 2
QD = 3
D1, D2, D3 = 2, 3, 5

OWN, MATE, LEFT, RIGHT, OPP = 0, 1, 2, 4, 6

KINDS = ('QR', 'QL', 'FR', 'FL', 'ML', 'MR', 'MO', 'S1', 'S2', 'S3', 'S4', 'S5', 'S6', 'S7',
         'MA', 'MB', 'MC', 'HR0', 'HR1', 'HL0', 'HL1', 'DR0', 'DR1', 'DL0', 'DL1', 'AR', 'AL')
SEM = {k: i for i, k in enumerate(KINDS)}
LSE_TO = {'S1': (0, 1, MATE), 'S2': (1, 0, LEFT), 'S3': (1, 1, LEFT + 1), 'S4': (-1, 0, RIGHT),
          'S5': (-1, 1, RIGHT + 1), 'S6': (2, 0, OPP), 'S7': (2, 1, OPP + 1)}


def kernel(n, len_ref, q_hbm, c_hbm, o_hbm,
           q_v, c_v, o_v, lse_v, wrow, wt, m_a, m_b, m_c, h_p, h_n, d_p, d_n, a_p, a_n, r_p, r_n, out_v,
           send, recv, qm_sem, q_sem, c_sem, o_sem):
    G = q_v.shape[0]
    lat = o_v.shape[3]
    heads = o_v.shape[2]
    hl = heads // n
    sl = c_v.shape[2]
    nc = n // 2
    me = lax.axis_index('dcp')
    chip = lax.div(me, 2)
    core = lax.rem(me, 2)

    def dev(dx, other):
        return 2 * lax.rem(chip + dx + nc, nc) + (1 - core if other else core)

    def hd(d):
        return pl.ds(pl.multiple_of(d * hl, hl), hl)

    first, second, both = pl.ds(0, H), pl.ds(H, H), pl.ds(0, SC)
    right, left, opp, mate = dev(1, 0), dev(-1, 0), dev(2, 0), dev(0, 1)
    right1, left1, opp1 = dev(1, 1), dev(-1, 1), dev(2, 1)

    def same_q(g, part, d):
        r = q_v.at[g, part, hd(d)]
        return r, r

    def msg(kind, g):
        if kind == 'QR':
            src, dst = same_q(g, both, me)
            to = right
        elif kind == 'QL':
            src, dst = same_q(g, both, me)
            to = left
        elif kind == 'FR':
            src, dst = same_q(g, first, left)
            to = right
        elif kind == 'FL':
            src, dst = same_q(g, second, right)
            to = left
        elif kind == 'ML':
            src, dst = same_q(g, both, left)
            to = mate
        elif kind == 'MR':
            src, dst = same_q(g, both, right)
            to = mate
        elif kind == 'MO':
            src, dst = same_q(g, both, opp)
            to = mate
        elif kind in LSE_TO:
            dx, other, slot = LSE_TO[kind]
            src, dst, to = lse_v.at[OWN, g], lse_v.at[slot, g], dev(dx, other)
        elif kind == 'MA':
            src, dst, to = o_v.at[g, both, hd(mate)], m_a.at[g], mate
        elif kind == 'MB':
            src, dst, to = o_v.at[g, first, hd(right1)], m_b.at[g], mate
        elif kind == 'MC':
            src, dst, to = o_v.at[g, second, hd(left1)], m_c.at[g], mate
        elif kind == 'HR0':
            src, dst, to = o_v.at[g, first, hd(opp)], h_p.at[0, g], right
        elif kind == 'HR1':
            src, dst, to = o_v.at[g, first, hd(opp1)], h_p.at[1, g], right1
        elif kind == 'HL0':
            src, dst, to = o_v.at[g, second, hd(opp)], h_n.at[0, g], left
        elif kind == 'HL1':
            src, dst, to = o_v.at[g, second, hd(opp1)], h_n.at[1, g], left1
        elif kind == 'DR0':
            src, dst, to = o_v.at[g, second, hd(right)], d_p.at[0, g], right
        elif kind == 'DR1':
            src, dst, to = o_v.at[g, second, hd(right1)], d_p.at[1, g], right1
        elif kind == 'DL0':
            src, dst, to = o_v.at[g, first, hd(left)], d_n.at[0, g], left
        elif kind == 'DL1':
            src, dst, to = o_v.at[g, first, hd(left1)], d_n.at[1, g], left1
        elif kind == 'AR':
            src, dst, to = a_p.at[g], r_p.at[g], right
        else:
            src, dst, to = a_n.at[g], r_n.at[g], left
        i = SEM[kind]
        return pltpu.make_async_remote_copy(
            src_ref=src, dst_ref=dst, send_sem=send.at[i, g], recv_sem=recv.at[i, g],
            device_id={'dcp': to}, device_id_type=pl.DeviceIdType.MESH)

    def start(g, *kinds):
        for k in kinds:
            msg(k, g).start()

    def arrived(g, *kinds):
        for k in kinds:
            msg(k, g).wait_recv()

    def load(g, i):
        slot = lax.rem(g, 2) * SC + i
        return pltpu.make_async_copy(c_hbm.at[g, i], c_v.at[slot], c_sem.at[slot])

    def result(g):
        return pltpu.make_async_copy(out_v.at[g], o_hbm.at[g], o_sem.at[g])

    own = pltpu.make_async_copy(q_hbm, q_v.at[:, :, hd(me)], q_sem)
    own.start()
    for g in range(min(2, G)):
        for i in range(SC):
            load(g, i).start()
    wrow[...] = jnp.zeros_like(wrow)

    barrier = pltpu.get_barrier_semaphore()
    for d in (mate, right, right1, left, left1, opp, opp1):
        pl.semaphore_signal(barrier, inc=1, device_id={'dcp': d}, device_id_type=pl.DeviceIdType.MESH)
    pl.semaphore_wait(barrier, n - 1)
    own.wait()

    qm_ref = q_v.at[:, :, hd(me)]
    to_mate = pltpu.make_async_remote_copy(
        src_ref=qm_ref, dst_ref=qm_ref, send_sem=qm_sem.at[0], recv_sem=qm_sem.at[1],
        device_id={'dcp': mate}, device_id_type=pl.DeviceIdType.MESH)
    for g in range(min(QD, G)):
        start(g, 'QR', 'QL')
    to_mate.start()

    def attention(g):
        for i in range(SC):
            load(g, i).wait()
        pos = me * sl + lax.broadcasted_iota(jnp.int32, (1, sl), 1)
        lane = lax.broadcasted_iota(jnp.int32, (heads, 128), 1)
        lses = jnp.zeros((heads, 128), F32)
        for i in range(SC):
            c = c_v.at[lax.rem(g, 2) * SC + i]
            s = jnp.dot(q_v[g, i], c[...], preferred_element_type=F32)
            s = jnp.where(pos < len_ref[g * SC + i], s * SCALE, -jnp.inf)
            m = jnp.max(s, axis=1, keepdims=True)
            m0 = jnp.where(m > -jnp.inf, m, 0.0)
            p = jnp.exp(s - m0)
            l = jnp.sum(p, axis=1, keepdims=True)
            pv = lax.dot_general(p.astype(BF16), c[:lat], NT, preferred_element_type=F32)
            has = l > 0.0
            l1 = jnp.where(has, l, 1.0)
            o_v[g, i] = (pv * (1.0 / l1)).astype(BF16)
            lse = jnp.where(has, m0 + jnp.log(l1), -jnp.inf)
            lses = jnp.where(lane == i, lse, lses)
        lse_v[OWN, g] = lses.T[:SC]

    def weights(g):
        ls = [lse_v[s, g] for s in range(n)]
        mx = functools.reduce(jnp.maximum, ls)
        es = [jnp.exp(x - mx) for x in ls]
        z = 1.0 / functools.reduce(jnp.add, es)
        for s in range(n):
            wrow[s * SC:(s + 1) * SC, :] = es[s] * z
        wt[g] = wrow[...].T

    def weighted(w, slot, i, o):
        c = slot * SC + i
        return w[:, c:c + 1] * o.astype(F32)

    def partial_sums(g):
        w = wt[g, hd(right)]
        for i in range(H):
            a_p[g, i] = (weighted(w, OWN, i, o_v[g, i, hd(right)]) + weighted(w, MATE, i, m_b[g, i])
                         + weighted(w, LEFT, i, h_p[0, g, i]) + weighted(w, LEFT + 1, i, h_p[1, g, i]))
        w = wt[g, hd(left)]
        for i in range(H):
            a_n[g, i] = (weighted(w, OWN, H + i, o_v[g, H + i, hd(left)]) + weighted(w, MATE, H + i, m_c[g, i])
                         + weighted(w, RIGHT, H + i, h_n[0, g, i]) + weighted(w, RIGHT + 1, H + i, h_n[1, g, i]))

    def final(g):
        w = wt[g, hd(me)]
        for i in range(SC):
            o = weighted(w, OWN, i, o_v[g, i, hd(me)]) + weighted(w, MATE, i, m_a[g, i])
            if i < H:
                o += (r_p[g, i] + weighted(w, RIGHT, i, d_n[0, g, i]) + weighted(w, RIGHT + 1, i, d_n[1, g, i]))
            else:
                j = i - H
                o += (r_n[g, j] + weighted(w, LEFT, i, d_p[0, g, j]) + weighted(w, LEFT + 1, i, d_p[1, g, j]))
            out_v[g, i] = o.astype(BF16)

    def stage(t, lag, extra=0):
        g = t - lag
        return g, (g >= 0) & (g < G - extra)

    def step(t, carry):
        a, on = stage(t, 0)

        @pl.when(on)
        def _():
            arrived(a, 'QR', 'QL')
            start(a, 'FR', 'FL', 'ML', 'MR')

        @pl.when(stage(t, 0, QD)[1])
        def _():
            start(t + QD, 'QR', 'QL')

        b, on = stage(t, 1)

        @pl.when(on)
        def _():
            arrived(b, 'FR', 'FL')
            start(b, 'MO')

        @pl.when(t == 2)
        def _():
            to_mate.wait_recv()

        g, on = stage(t, 2)

        @pl.when(on)
        def _():
            arrived(g, 'ML', 'MR', 'MO')
            attention(g)
            start(g, 'HR0', 'HR1', 'HL0', 'HL1', 'MA', 'MB', 'MC', *LSE_TO)

        @pl.when(stage(t, 2, 2)[1])
        def _():
            for i in range(SC):
                load(t, i).start()

        d, on = stage(t, 2 + D1)

        @pl.when(on)
        def _():
            arrived(d, 'HR0', 'HR1', 'HL0', 'HL1', 'MB', 'MC', *LSE_TO)
            weights(d)
            partial_sums(d)
            start(d, 'AR', 'AL')

        e, on = stage(t, 2 + D2)

        @pl.when(on)
        def _():
            start(e, 'DR0', 'DR1', 'DL0', 'DL1')

        f, on = stage(t, 2 + D3)

        @pl.when(on)
        def _():
            arrived(f, 'MA', 'AR', 'AL', 'DR0', 'DR1', 'DL0', 'DL1')
            final(f)
            result(f).start()

        f, on = stage(t, 3 + D3)

        @pl.when(on)
        def _():
            for k in KINDS:
                msg(k, f).wait_send()
            result(f).wait()

        return carry

    lax.fori_loop(0, G + 4 + D3, step, 0)
    to_mate.wait_send()


def solution(mesh):
    n = mesh.shape['dcp']

    def local(q, cache, lengths):
        b, sl, wd = cache.shape
        hl = q.shape[1]
        heads = hl * n
        lat = wd - ROPE
        G = b // SC
        ct = jnp.swapaxes(cache, 1, 2).reshape(G, SC, wd, sl)
        vmem = pltpu.VMEM
        out = pl.pallas_call(
            functools.partial(kernel, n),
            out_shape=jax.ShapeDtypeStruct((G, SC, hl, lat), BF16),
            in_specs=[pl.BlockSpec(memory_space=pltpu.SMEM), pl.BlockSpec(memory_space=pl.ANY),
                      pl.BlockSpec(memory_space=pl.ANY)],
            out_specs=pl.BlockSpec(memory_space=pl.ANY),
            scratch_shapes=[
                vmem((G, SC, heads, wd), BF16),
                vmem((2 * SC, wd, sl), BF16),
                vmem((G, SC, heads, lat), BF16),
                vmem((n, G, SC, heads), F32),
                vmem((128, heads), F32),
                vmem((G, heads, 128), F32),
                vmem((G, SC, hl, lat), BF16),
                vmem((G, H, hl, lat), BF16),
                vmem((G, H, hl, lat), BF16),
                vmem((2, G, H, hl, lat), BF16),
                vmem((2, G, H, hl, lat), BF16),
                vmem((2, G, H, hl, lat), BF16),
                vmem((2, G, H, hl, lat), BF16),
                vmem((G, H, hl, lat), F32),
                vmem((G, H, hl, lat), F32),
                vmem((G, H, hl, lat), F32),
                vmem((G, H, hl, lat), F32),
                vmem((G, SC, hl, lat), BF16),
                pltpu.SemaphoreType.DMA((len(KINDS), G)),
                pltpu.SemaphoreType.DMA((len(KINDS), G)),
                pltpu.SemaphoreType.DMA((2,)),
                pltpu.SemaphoreType.DMA,
                pltpu.SemaphoreType.DMA((2 * SC,)),
                pltpu.SemaphoreType.DMA((G,)),
            ],
            compiler_params=pltpu.CompilerParams(
                collective_id=0, has_side_effects=True, vmem_limit_bytes=56 * 2 ** 20),
        )(lengths, q.reshape(G, SC, hl, wd), ct)
        return out.reshape(b, hl, lat)

    return jax.shard_map(local, mesh=mesh, in_specs=(P('dp', 'dcp', None), P('dp', 'dcp', None), P('dp')),
                         out_specs=P('dp', 'dcp', None), check_vma=False)
```

```python
import functools

import jax
import jax.numpy as jnp
from jax import lax
from jax.experimental import pallas as pl
from jax.experimental.pallas import tpu as pltpu
from jax.sharding import PartitionSpec as P

ROPE = 64
SCALE = 192 ** -0.5
F32 = jnp.float32
BF16 = jnp.bfloat16
NT = (((1,), (1,)), ((), ()))

SC = 4
H = SC // 2
QD = 3
D1, D2 = 2, 2

OWN, MATE, LEFT, RIGHT = 0, 1, 2, 4

KINDS = ('QR', 'QL', 'FR', 'FL', 'ML', 'MR', 'MO', 'QM', 'S1', 'S2', 'S3', 'S4', 'S5', 'TR', 'TL',
         'MA', 'MB', 'MC', 'HR0', 'HR1', 'HL0', 'HL1', 'DR0', 'DR1', 'DL0', 'DL1', 'AR', 'AL')
SEM = {k: i for i, k in enumerate(KINDS)}
LSE_TO = {'S1': (0, 1, MATE), 'S2': (1, 0, LEFT), 'S3': (1, 1, LEFT + 1), 'S4': (-1, 0, RIGHT),
          'S5': (-1, 1, RIGHT + 1)}


def kernel(n, len_hbm, q_hbm, c_hbm, out_v,
           len_ref, q_st, q_v, c_v, o_v, lse_v, t_s, t_r, wrow, wt, m_a, m_b, m_c, h_p, h_n, d_p, d_n, a_p, a_n, r_p, r_n,
           send, recv, len_sem, q_sem, c_sem):
    G = q_v.shape[0]
    lat = o_v.shape[3]
    heads = o_v.shape[2]
    hl = heads // n
    sl = c_v.shape[2]
    nc = n // 2
    me = lax.axis_index('dcp')
    chip = lax.div(me, 2)
    core = lax.rem(me, 2)

    def dev(dx, other):
        return 2 * lax.rem(chip + dx + nc, nc) + (1 - core if other else core)

    def hd(d):
        return pl.ds(pl.multiple_of(d * hl, hl), hl)

    first, second, both = pl.ds(0, H), pl.ds(H, H), pl.ds(0, SC)
    pairs, pairs1, pairs2 = pl.ds(0, H), pl.ds(0, H // 2), pl.ds(H // 2, H // 2)
    right, left, opp, mate = dev(1, 0), dev(-1, 0), dev(2, 0), dev(0, 1)
    right1, left1, opp1 = dev(1, 1), dev(-1, 1), dev(2, 1)

    def same_q(g, part, d):
        r = q_v.at[g, part, hd(d)]
        return r, r

    def msg(kind, g):
        if kind == 'QR':
            src, dst = same_q(g, pairs, me)
            to = right
        elif kind == 'QL':
            src, dst = same_q(g, pairs, me)
            to = left
        elif kind == 'FR':
            src, dst = same_q(g, pairs1, left)
            to = right
        elif kind == 'FL':
            src, dst = same_q(g, pairs2, right)
            to = left
        elif kind == 'ML':
            src, dst = same_q(g, pairs, left)
            to = mate
        elif kind == 'MR':
            src, dst = same_q(g, pairs, right)
            to = mate
        elif kind == 'MO':
            src, dst = same_q(g, pairs, opp)
            to = mate
        elif kind == 'QM':
            src, dst = same_q(g, pairs, me)
            to = mate
        elif kind == 'TR':
            src, dst, to = t_s.at[0, g], t_r.at[0, g], right
        elif kind == 'TL':
            src, dst, to = t_s.at[1, g], t_r.at[1, g], left
        elif kind in LSE_TO:
            dx, other, slot = LSE_TO[kind]
            src, dst, to = lse_v.at[OWN, g], lse_v.at[slot, g], dev(dx, other)
        elif kind == 'MA':
            src, dst, to = o_v.at[g, both, hd(mate)], m_a.at[g], mate
        elif kind == 'MB':
            src, dst, to = o_v.at[g, first, hd(right1)], m_b.at[g], mate
        elif kind == 'MC':
            src, dst, to = o_v.at[g, second, hd(left1)], m_c.at[g], mate
        elif kind == 'HR0':
            src, dst, to = o_v.at[g, first, hd(opp)], h_p.at[0, g], right
        elif kind == 'HR1':
            src, dst, to = o_v.at[g, first, hd(opp1)], h_p.at[1, g], right1
        elif kind == 'HL0':
            src, dst, to = o_v.at[g, second, hd(opp)], h_n.at[0, g], left
        elif kind == 'HL1':
            src, dst, to = o_v.at[g, second, hd(opp1)], h_n.at[1, g], left1
        elif kind == 'DR0':
            src, dst, to = o_v.at[g, second, hd(right)], d_p.at[0, g], right
        elif kind == 'DR1':
            src, dst, to = o_v.at[g, second, hd(right1)], d_p.at[1, g], right1
        elif kind == 'DL0':
            src, dst, to = o_v.at[g, first, hd(left)], d_n.at[0, g], left
        elif kind == 'DL1':
            src, dst, to = o_v.at[g, first, hd(left1)], d_n.at[1, g], left1
        elif kind == 'AR':
            src, dst, to = a_p.at[g], r_p.at[g], right
        else:
            src, dst, to = a_n.at[g], r_n.at[g], left
        i = SEM[kind]
        return pltpu.make_async_remote_copy(
            src_ref=src, dst_ref=dst, send_sem=send.at[i, g], recv_sem=recv.at[i, g],
            device_id={'dcp': to}, device_id_type=pl.DeviceIdType.MESH)

    def start(g, *kinds):
        for k in kinds:
            msg(k, g).start()

    def arrived(g, *kinds):
        for k in kinds:
            msg(k, g).wait_recv()

    def load(g, i):
        slot = lax.rem(g, 2) * SC + i
        return pltpu.make_async_copy(c_hbm.at[g, i], c_v.at[slot], c_sem.at[slot])

    barrier = pltpu.get_barrier_semaphore()
    for d in (mate, right, right1, left, left1):
        pl.semaphore_signal(barrier, inc=1, device_id={'dcp': d}, device_id_type=pl.DeviceIdType.MESH)

    def fetch(g):
        return pltpu.make_async_copy(q_hbm.at[g], q_st.at[g], q_sem.at[g])

    def fetch_start(g, carry):
        fetch(g).start()
        return carry

    lax.fori_loop(0, G, fetch_start, 0)
    lens = pltpu.make_async_copy(len_hbm, len_ref, len_sem)
    lens.start()
    for g in range(min(2, G)):
        for i in range(SC):
            load(g, i).start()
    wrow[...] = jnp.zeros_like(wrow)

    def pack(g):
        fetch(g).wait()
        for p in range(H):
            a, b = q_st[g, 2 * p], q_st[g, 2 * p + 1]
            q_v[g, p, hd(me), :lat] = a[:, :lat]
            q_v[g, p, hd(me), lat:2 * lat] = b[:, :lat]
            q_v[g, p, hd(me), 2 * lat:] = jnp.concatenate([a[:, lat:], b[:, lat:]], axis=1)

    for g in range(min(QD, G)):
        pack(g)
    lens.wait()
    pl.semaphore_wait(barrier, 5)
    for g in range(min(QD, G)):
        start(g, 'QR', 'QL', 'QM')

    def attention(g):
        for i in range(SC):
            load(g, i).wait()
        pos = me * sl + lax.broadcasted_iota(jnp.int32, (1, sl), 1)
        lane = lax.broadcasted_iota(jnp.int32, (heads, 128), 1)
        lses = jnp.zeros((heads, 128), F32)
        for i in range(SC):
            c = c_v.at[lax.rem(g, 2) * SC + i]
            p, r = divmod(i, 2)
            rope = q_v[g, p, :, 2 * lat + r * ROPE:2 * lat + (r + 1) * ROPE]
            s = (jnp.dot(q_v[g, p, :, r * lat:(r + 1) * lat], c[:lat], preferred_element_type=F32)
                 + jnp.dot(rope, c[lat:], preferred_element_type=F32))
            s = jnp.where(pos < len_ref[g * SC + i], s * SCALE, -jnp.inf)
            m = jnp.max(s, axis=1, keepdims=True)
            m0 = jnp.where(m > -jnp.inf, m, 0.0)
            p = jnp.exp(s - m0)
            l = jnp.sum(p, axis=1, keepdims=True)
            pv = lax.dot_general(p.astype(BF16), c[:lat], NT, preferred_element_type=F32)
            has = l > 0.0
            l1 = jnp.where(has, l, 1.0)
            o_v[g, i] = (pv * (1.0 / l1)).astype(BF16)
            lse = jnp.where(has, m0 + jnp.log(l1), -jnp.inf)
            lses = jnp.where(lane == i, lse, lses)
        lse_v[OWN, g] = lses.T[:SC]

    row = lax.broadcasted_iota(jnp.int32, (SC, heads), 0)

    def softmax(ls):
        mx = functools.reduce(jnp.maximum, ls)
        mx = jnp.where(mx > -jnp.inf, mx, 0.0)
        es = [jnp.exp(x - mx) for x in ls]
        z = functools.reduce(jnp.add, es)
        has = z > 0.0
        z1 = jnp.where(has, z, 1.0)
        r = 1.0 / z1
        for k, e in enumerate(es):
            wrow[k * SC:(k + 1) * SC, :] = e * r
        wt[...] = wrow[...].T
        return jnp.where(has, mx + jnp.log(z1), -jnp.inf)

    def near(g, k, a, b):
        return jnp.where(row < H, lse_v[a + k, g], lse_v[b + k, g])

    def weighted(w, k, i, o):
        c = k * SC + i
        return w[:, c:c + 1] * o.astype(F32)

    def partial_sums(g):
        t = softmax([lse_v[OWN, g], lse_v[MATE, g], near(g, 0, LEFT, RIGHT), near(g, 1, LEFT, RIGHT)])
        t_s[0, g] = t[:H]
        t_s[1, g] = t[H:]
        for first_half, d, m, h, a in ((True, right, m_b, h_p, a_p), (False, left, m_c, h_n, a_n)):
            w = wt[hd(d)]
            for j in range(H):
                i = j if first_half else H + j
                a[g, j] = (weighted(w, 0, i, o_v[g, i, hd(d)]) + weighted(w, 1, i, m[g, j])
                           + weighted(w, 2, i, h[0, g, j]) + weighted(w, 3, i, h[1, g, j]))

    def final(g):
        far = jnp.concatenate([t_r[0, g], t_r[1, g]], axis=0)
        softmax([lse_v[OWN, g], lse_v[MATE, g], near(g, 0, RIGHT, LEFT), near(g, 1, RIGHT, LEFT), far])
        w = wt[hd(me)]
        for i in range(SC):
            d, r, j = (d_n, r_p, i) if i < H else (d_p, r_n, i - H)
            out_v[g, i] = (weighted(w, 0, i, o_v[g, i, hd(me)]) + weighted(w, 1, i, m_a[g, i])
                           + weighted(w, 2, i, d[0, g, j]) + weighted(w, 3, i, d[1, g, j])
                           + weighted(w, 4, i, r[g, j])).astype(BF16)

    def stage(t, lag, extra=0):
        g = t - lag
        return g, (g >= 0) & (g < G - extra)

    def step(t, carry):
        a, on = stage(t, 0)

        @pl.when(on)
        def _():
            arrived(a, 'QR', 'QL')
            start(a, 'FR', 'FL', 'ML', 'MR')

        @pl.when(stage(t, 0, QD)[1])
        def _():
            pack(t + QD)
            start(t + QD, 'QR', 'QL', 'QM')

        b, on = stage(t, 1)

        @pl.when(on)
        def _():
            arrived(b, 'FR', 'FL')
            start(b, 'MO')

        g, on = stage(t, 2)

        @pl.when(on)
        def _():
            arrived(g, 'QM', 'ML', 'MR', 'MO')
            attention(g)
            start(g, 'HR0', 'HR1', 'HL0', 'HL1', 'MA', 'MB', 'MC', *LSE_TO)

        @pl.when(stage(t, 2, 2)[1])
        def _():
            for i in range(SC):
                load(t, i).start()

        d, on = stage(t, 2 + D1)

        @pl.when(on)
        def _():
            sums(d)

        e, on = stage(t, 2 + D2)

        @pl.when(on)
        def _():
            start(e, 'DR0', 'DR1', 'DL0', 'DL1')

        return carry

    def sums(g):
        arrived(g, 'HR0', 'HR1', 'HL0', 'HL1', 'MB', 'MC', *LSE_TO)
        partial_sums(g)
        start(g, 'AR', 'AL', 'TR', 'TL')

    lax.fori_loop(0, G + 2, step, 0)

    def direct(g, carry):
        start(g, 'DR0', 'DR1', 'DL0', 'DL1')
        return carry

    lax.fori_loop(G - D2, G, direct, 0)

    def rest(g, carry):
        sums(g)
        return carry

    lax.fori_loop(G - D1, G, rest, 0)

    def sent(g):
        for k in KINDS:
            msg(k, g).wait_send()

    def finish(g, carry):
        @pl.when(g >= 1)
        def _():
            sent(g - 1)

        arrived(g, 'MA', 'AR', 'AL', 'TR', 'TL', 'DR0', 'DR1', 'DL0', 'DL1')
        final(g)
        return carry

    lax.fori_loop(0, G, finish, 0)
    sent(G - 1)


def solution(mesh):
    n = mesh.shape['dcp']

    def local(q, cache, lengths):
        b, sl, wd = cache.shape
        hl = q.shape[1]
        heads = hl * n
        lat = wd - ROPE
        G = b // SC
        ct = jnp.swapaxes(cache, 1, 2).reshape(G, SC, wd, sl)
        vmem = pltpu.VMEM
        out = pl.pallas_call(
            functools.partial(kernel, n),
            out_shape=vmem((G, SC, hl, lat), BF16),
            in_specs=[pl.BlockSpec(memory_space=pl.ANY)] * 3,
            out_specs=pl.BlockSpec(memory_space=pltpu.VMEM),
            scratch_shapes=[
                pltpu.SMEM((b,), jnp.int32),
                vmem((G, SC, hl, wd), BF16),
                vmem((G, H, heads, 2 * wd), BF16),
                vmem((2 * SC, wd, sl), BF16),
                vmem((G, SC, heads, lat), BF16),
                vmem((6, G, SC, heads), F32),
                vmem((2, G, H, heads), F32),
                vmem((2, G, H, heads), F32),
                vmem((128, heads), F32),
                vmem((heads, 128), F32),
                vmem((G, SC, hl, lat), BF16),
                vmem((G, H, hl, lat), BF16),
                vmem((G, H, hl, lat), BF16),
                vmem((2, G, H, hl, lat), BF16),
                vmem((2, G, H, hl, lat), BF16),
                vmem((2, G, H, hl, lat), BF16),
                vmem((2, G, H, hl, lat), BF16),
                vmem((G, H, hl, lat), F32),
                vmem((G, H, hl, lat), F32),
                vmem((G, H, hl, lat), F32),
                vmem((G, H, hl, lat), F32),
                pltpu.SemaphoreType.DMA((len(KINDS), G)),
                pltpu.SemaphoreType.DMA((len(KINDS), G)),
                pltpu.SemaphoreType.DMA,
                pltpu.SemaphoreType.DMA((G,)),
                pltpu.SemaphoreType.DMA((2 * SC,)),
            ],
            compiler_params=pltpu.CompilerParams(
                collective_id=0, has_side_effects=True, vmem_limit_bytes=56 * 2 ** 20),
        )(lengths, q.reshape(G, SC, hl, wd), ct)
        return out.reshape(b, hl, lat)

    return jax.shard_map(local, mesh=mesh, in_specs=(P('dp', 'dcp', None), P('dp', 'dcp', None), P('dp')),
                         out_specs=P('dp', 'dcp', None), check_vma=False)
```

```python
import functools

import jax
import jax.numpy as jnp
from jax import lax
from jax.experimental import pallas as pl
from jax.experimental.pallas import tpu as pltpu
from jax.sharding import PartitionSpec as P

ROPE = 64
SCALE = 192 ** -0.5
F32 = jnp.float32
BF16 = jnp.bfloat16
NT = (((1,), (1,)), ((), ()))

SC = 4
H = SC // 2
OWN_AT = {6: 2}
QD = 3
D1, D2 = 2, 2

OWN, MATE, LEFT, RIGHT = 0, 1, 2, 4

KINDS = ('QR', 'QL', 'FR', 'FL', 'ML', 'MR', 'MO', 'QM', 'S1', 'S2', 'S3', 'S4', 'S5', 'TR', 'TL',
         'MA', 'MB', 'MC', 'HR0', 'HR1', 'HL0', 'HL1', 'DR0', 'DR1', 'DL0', 'DL1', 'AR', 'AL')
SEM = {k: i for i, k in enumerate(KINDS)}
LSE_TO = {'S1': (0, 1, MATE), 'S2': (1, 0, LEFT), 'S3': (1, 1, LEFT + 1), 'S4': (-1, 0, RIGHT),
          'S5': (-1, 1, RIGHT + 1)}


def kernel(n, len_hbm, q_hbm, c_hbm, out_v,
           len_ref, q_st, q_v, c_v, o_v, lse_v, t_s, t_r, wrow, wt, m_a, m_b, m_c, h_p, h_n, d_p, d_n, a_p, a_n, r_p, r_n,
           send, recv, len_sem, q_sem, c_sem):
    G = q_v.shape[0]
    lat = o_v.shape[3]
    heads = o_v.shape[2]
    hl = heads // n
    sl = c_v.shape[2]
    nc = n // 2
    me = lax.axis_index('dcp')
    chip = lax.div(me, 2)
    core = lax.rem(me, 2)

    def dev(dx, other):
        return 2 * lax.rem(chip + dx + nc, nc) + (1 - core if other else core)

    def hd(d):
        return pl.ds(pl.multiple_of(d * hl, hl), hl)

    first, second, both = pl.ds(0, H), pl.ds(H, H), pl.ds(0, SC)
    pairs, pairs1, pairs2 = pl.ds(0, H), pl.ds(0, H // 2), pl.ds(H // 2, H // 2)
    right, left, opp, mate = dev(1, 0), dev(-1, 0), dev(2, 0), dev(0, 1)
    right1, left1, opp1 = dev(1, 1), dev(-1, 1), dev(2, 1)

    def same_q(g, part, d):
        r = q_v.at[g, part, hd(d)]
        return r, r

    def msg(kind, g):
        if kind == 'QR':
            src, dst = same_q(g, pairs, me)
            to = right
        elif kind == 'QL':
            src, dst = same_q(g, pairs, me)
            to = left
        elif kind == 'FR':
            src, dst = same_q(g, pairs1, left)
            to = right
        elif kind == 'FL':
            src, dst = same_q(g, pairs2, right)
            to = left
        elif kind == 'ML':
            src, dst = same_q(g, pairs, left)
            to = mate
        elif kind == 'MR':
            src, dst = same_q(g, pairs, right)
            to = mate
        elif kind == 'MO':
            src, dst = same_q(g, pairs, opp)
            to = mate
        elif kind == 'QM':
            src, dst = same_q(g, pairs, me)
            to = mate
        elif kind == 'TR':
            src, dst, to = t_s.at[0, g], t_r.at[0, g], right
        elif kind == 'TL':
            src, dst, to = t_s.at[1, g], t_r.at[1, g], left
        elif kind in LSE_TO:
            dx, other, slot = LSE_TO[kind]
            src, dst, to = lse_v.at[OWN, g], lse_v.at[slot, g], dev(dx, other)
        elif kind == 'MA':
            src, dst, to = o_v.at[g, both, hd(mate)], m_a.at[g], mate
        elif kind == 'MB':
            src, dst, to = o_v.at[g, first, hd(right1)], m_b.at[g], mate
        elif kind == 'MC':
            src, dst, to = o_v.at[g, second, hd(left1)], m_c.at[g], mate
        elif kind == 'HR0':
            src, dst, to = o_v.at[g, first, hd(opp)], h_p.at[0, g], right
        elif kind == 'HR1':
            src, dst, to = o_v.at[g, first, hd(opp1)], h_p.at[1, g], right1
        elif kind == 'HL0':
            src, dst, to = o_v.at[g, second, hd(opp)], h_n.at[0, g], left
        elif kind == 'HL1':
            src, dst, to = o_v.at[g, second, hd(opp1)], h_n.at[1, g], left1
        elif kind == 'DR0':
            src, dst, to = o_v.at[g, second, hd(right)], d_p.at[0, g], right
        elif kind == 'DR1':
            src, dst, to = o_v.at[g, second, hd(right1)], d_p.at[1, g], right1
        elif kind == 'DL0':
            src, dst, to = o_v.at[g, first, hd(left)], d_n.at[0, g], left
        elif kind == 'DL1':
            src, dst, to = o_v.at[g, first, hd(left1)], d_n.at[1, g], left1
        elif kind == 'AR':
            src, dst, to = a_p.at[g], r_p.at[g], right
        else:
            src, dst, to = a_n.at[g], r_n.at[g], left
        i = SEM[kind]
        return pltpu.make_async_remote_copy(
            src_ref=src, dst_ref=dst, send_sem=send.at[i, g], recv_sem=recv.at[i, g],
            device_id={'dcp': to}, device_id_type=pl.DeviceIdType.MESH)

    def start(g, *kinds):
        for k in kinds:
            msg(k, g).start()

    def arrived(g, *kinds):
        for k in kinds:
            msg(k, g).wait_recv()

    def load(g, i):
        slot = lax.rem(g, 2) * SC + i
        return pltpu.make_async_copy(c_hbm.at[g, i], c_v.at[slot], c_sem.at[slot])

    barrier = pltpu.get_barrier_semaphore()
    for d in (mate, right, right1, left, left1):
        pl.semaphore_signal(barrier, inc=1, device_id={'dcp': d}, device_id_type=pl.DeviceIdType.MESH)

    def fetch(g):
        return pltpu.make_async_copy(q_hbm.at[g], q_st.at[g], q_sem.at[g])

    def fetch_start(g, carry):
        fetch(g).start()
        return carry

    lax.fori_loop(0, G, fetch_start, 0)
    lens = pltpu.make_async_copy(len_hbm, len_ref, len_sem)
    lens.start()
    for g in range(min(2, G)):
        for i in range(SC):
            load(g, i).start()
    wrow[...] = jnp.zeros_like(wrow)

    def pack(g):
        fetch(g).wait()
        for p in range(H):
            a, b = q_st[g, 2 * p], q_st[g, 2 * p + 1]
            q_v[g, p, hd(me), :lat] = a[:, :lat]
            q_v[g, p, hd(me), lat:2 * lat] = b[:, :lat]
            q_v[g, p, hd(me), 2 * lat:] = jnp.concatenate([a[:, lat:], b[:, lat:]], axis=1)

    for g in range(min(QD, G)):
        pack(g)
    lens.wait()
    pl.semaphore_wait(barrier, 5)
    for g in range(min(QD, G)):
        start(g, 'QR', 'QL', 'QM')

    def attention(g):
        for i in range(SC):
            load(g, i).wait()
        pos = me * sl + lax.broadcasted_iota(jnp.int32, (1, sl), 1)
        lane = lax.broadcasted_iota(jnp.int32, (heads, 128), 1)
        lses = jnp.zeros((heads, 128), F32)

        def scores(i):
            c = c_v.at[lax.rem(g, 2) * SC + i]
            p, r = divmod(i, 2)
            rope = q_v[g, p, :, 2 * lat + r * ROPE:2 * lat + (r + 1) * ROPE]
            return (jnp.dot(q_v[g, p, :, r * lat:(r + 1) * lat], c[:lat], preferred_element_type=F32)
                    + jnp.dot(rope, c[lat:], preferred_element_type=F32))

        ahead = scores(0)
        for i in range(SC):
            c = c_v.at[lax.rem(g, 2) * SC + i]
            s, ahead = ahead, scores(i + 1) if i + 1 < SC else None
            s = jnp.where(pos < len_ref[g * SC + i], s * SCALE, -jnp.inf)
            m = jnp.max(s, axis=1, keepdims=True)
            m0 = jnp.where(m > -jnp.inf, m, 0.0)
            p = jnp.exp(s - m0)
            l = jnp.sum(p, axis=1, keepdims=True)
            pv = lax.dot_general(p.astype(BF16), c[:lat], NT, preferred_element_type=F32)
            has = l > 0.0
            l1 = jnp.where(has, l, 1.0)
            o_v[g, i] = (pv * (1.0 / l1)).astype(BF16)
            lse = jnp.where(has, m0 + jnp.log(l1), -jnp.inf)
            lses = jnp.where(lane == i, lse, lses)
        lse_v[OWN, g] = lses.T[:SC]

    row = lax.broadcasted_iota(jnp.int32, (SC, heads), 0)

    def softmax(ls):
        mx = functools.reduce(jnp.maximum, ls)
        mx = jnp.where(mx > -jnp.inf, mx, 0.0)
        es = [jnp.exp(x - mx) for x in ls]
        z = functools.reduce(jnp.add, es)
        has = z > 0.0
        z1 = jnp.where(has, z, 1.0)
        r = 1.0 / z1
        for k, e in enumerate(es):
            wrow[k * SC:(k + 1) * SC, :] = e * r
        wt[...] = wrow[...].T
        return jnp.where(has, mx + jnp.log(z1), -jnp.inf)

    def near(g, k, a, b):
        return jnp.where(row < H, lse_v[a + k, g], lse_v[b + k, g])

    def weighted(w, k, i, o):
        c = k * SC + i
        return w[:, c:c + 1] * o.astype(F32)

    def partial_sums(g):
        t = softmax([lse_v[OWN, g], lse_v[MATE, g], near(g, 0, LEFT, RIGHT), near(g, 1, LEFT, RIGHT)])
        t_s[0, g] = t[:H]
        t_s[1, g] = t[H:]
        for first_half, d, m, h, a in ((True, right, m_b, h_p, a_p), (False, left, m_c, h_n, a_n)):
            w = wt[hd(d)]
            for j in range(H):
                i = j if first_half else H + j
                a[g, j] = (weighted(w, 0, i, o_v[g, i, hd(d)]) + weighted(w, 1, i, m[g, j])
                           + weighted(w, 2, i, h[0, g, j]) + weighted(w, 3, i, h[1, g, j]))

    def final(g):
        far = jnp.concatenate([t_r[0, g], t_r[1, g]], axis=0)
        softmax([lse_v[OWN, g], lse_v[MATE, g], near(g, 0, RIGHT, LEFT), near(g, 1, RIGHT, LEFT), far])
        w = wt[hd(me)]
        for i in range(SC):
            d, r, j = (d_n, r_p, i) if i < H else (d_p, r_n, i - H)
            out_v[g, i] = (weighted(w, 0, i, o_v[g, i, hd(me)]) + weighted(w, 1, i, m_a[g, i])
                           + weighted(w, 2, i, d[0, g, j]) + weighted(w, 3, i, d[1, g, j])
                           + weighted(w, 4, i, r[g, j])).astype(BF16)

    def stage(t, lag, extra=0):
        g = t - lag
        return g, (g >= 0) & (g < G - extra)

    def step(t, carry):
        a, on = stage(t, 0)

        @pl.when(on)
        def _():
            arrived(a, 'QR', 'QL')
            start(a, 'FR', 'FL', 'ML', 'MR')

        for h in range(QD, G):
            @pl.when(t == OWN_AT.get(h, h - QD))
            def _():
                pack(h)
                start(h, 'QR', 'QL', 'QM')

        b, on = stage(t, 1)

        @pl.when(on)
        def _():
            arrived(b, 'FR', 'FL')
            start(b, 'MO')

        e, on = stage(t, 2 + D2)

        @pl.when(on)
        def _():
            start(e, 'DR0', 'DR1', 'DL0', 'DL1')

        g, on = stage(t, 2)

        @pl.when(on)
        def _():
            arrived(g, 'QM', 'ML', 'MR', 'MO')
            attention(g)
            start(g, 'HR0', 'HR1', 'HL0', 'HL1', 'MA', 'MB', 'MC', *LSE_TO)

        @pl.when(stage(t, 2, 2)[1])
        def _():
            for i in range(SC):
                load(t, i).start()

        d, on = stage(t, 2 + D1)

        @pl.when(on)
        def _():
            sums(d)

        return carry

    def sums(g):
        arrived(g, 'HR0', 'HR1', 'HL0', 'HL1', 'MB', 'MC', *LSE_TO)
        partial_sums(g)
        start(g, 'AR', 'AL', 'TR', 'TL')

    lax.fori_loop(0, G + 2, step, 0)

    def direct(g, carry):
        start(g, 'DR0', 'DR1', 'DL0', 'DL1')
        return carry

    lax.fori_loop(G - D2, G, direct, 0)

    def rest(g, carry):
        sums(g)
        return carry

    lax.fori_loop(G - D1, G, rest, 0)

    def sent(g):
        for k in KINDS:
            msg(k, g).wait_send()

    def finish(g, carry):
        @pl.when(g >= 1)
        def _():
            sent(g - 1)

        arrived(g, 'MA', 'AR', 'AL', 'TR', 'TL', 'DR0', 'DR1', 'DL0', 'DL1')
        final(g)
        return carry

    lax.fori_loop(0, G, finish, 0)
    sent(G - 1)


def solution(mesh):
    n = mesh.shape['dcp']

    def local(q, cache, lengths):
        b, sl, wd = cache.shape
        hl = q.shape[1]
        heads = hl * n
        lat = wd - ROPE
        G = b // SC
        ct = jnp.swapaxes(cache, 1, 2).reshape(G, SC, wd, sl)
        vmem = pltpu.VMEM
        out = pl.pallas_call(
            functools.partial(kernel, n),
            out_shape=vmem((G, SC, hl, lat), BF16),
            in_specs=[pl.BlockSpec(memory_space=pl.ANY)] * 3,
            out_specs=pl.BlockSpec(memory_space=pltpu.VMEM),
            scratch_shapes=[
                pltpu.SMEM((b,), jnp.int32),
                vmem((G, SC, hl, wd), BF16),
                vmem((G, H, heads, 2 * wd), BF16),
                vmem((2 * SC, wd, sl), BF16),
                vmem((G, SC, heads, lat), BF16),
                vmem((6, G, SC, heads), F32),
                vmem((2, G, H, heads), F32),
                vmem((2, G, H, heads), F32),
                vmem((128, heads), F32),
                vmem((heads, 128), F32),
                vmem((G, SC, hl, lat), BF16),
                vmem((G, H, hl, lat), BF16),
                vmem((G, H, hl, lat), BF16),
                vmem((2, G, H, hl, lat), BF16),
                vmem((2, G, H, hl, lat), BF16),
                vmem((2, G, H, hl, lat), BF16),
                vmem((2, G, H, hl, lat), BF16),
                vmem((G, H, hl, lat), F32),
                vmem((G, H, hl, lat), F32),
                vmem((G, H, hl, lat), F32),
                vmem((G, H, hl, lat), F32),
                pltpu.SemaphoreType.DMA((len(KINDS), G)),
                pltpu.SemaphoreType.DMA((len(KINDS), G)),
                pltpu.SemaphoreType.DMA,
                pltpu.SemaphoreType.DMA((G,)),
                pltpu.SemaphoreType.DMA((2 * SC,)),
            ],
            compiler_params=pltpu.CompilerParams(
                collective_id=0, has_side_effects=True, vmem_limit_bytes=56 * 2 ** 20),
        )(lengths, q.reshape(G, SC, hl, wd), ct)
        return out.reshape(b, hl, lat)

    return jax.shard_map(local, mesh=mesh, in_specs=(P('dp', 'dcp', None), P('dp', 'dcp', None), P('dp')),
                         out_specs=P('dp', 'dcp', None), check_vma=False)
```

```python
import functools

import jax
import jax.numpy as jnp
from jax import lax
from jax.experimental import pallas as pl
from jax.experimental.pallas import tpu as pltpu
from jax.sharding import PartitionSpec as P

ROPE = 64
SCALE = 192 ** -0.5
F32 = jnp.float32
BF16 = jnp.bfloat16
NT = (((1,), (1,)), ((), ()))

SC = 4
H = SC // 2
OWN_AT = {6: 2, 7: 3}
QD = 3
D1, D2 = 2, 2

ROWS = ((1, -1), (0, 0), (2, 1), (-1, 2))

KINDS = ('QR', 'QL', 'FR', 'FL', 'ML', 'MR', 'MO', 'QM', 'S1', 'S2', 'S3', 'S4', 'S5', 'TR', 'TL',
         'MA', 'MB', 'MC', 'HR0', 'HR1', 'HL0', 'HL1', 'DR0', 'DR1', 'DL0', 'DL1', 'AR', 'AL')
SEM = {k: i for i, k in enumerate(KINDS)}

def kernel(n, len_hbm, q_hbm, c_hbm, out_v,
           len_ref, q_st, q_v, c_v, o_v, lse_c, z_own, z_mate, y_s, y_l, y_r, t_s, t_l, t_r, wrow, wt, m_a, m_b, m_c, h_p, h_n, d_p, d_n, a_p, a_n, r_p, r_n,
           send, recv, len_sem, q_sem, c_sem):
    G = q_v.shape[0]
    lat = o_v.shape[3]
    heads = o_v.shape[2]
    hl = heads // n
    sl = c_v.shape[2]
    nc = n // 2
    me = lax.axis_index('dcp')
    chip = lax.div(me, 2)
    core = lax.rem(me, 2)

    def dev(dx, other):
        return 2 * lax.rem(chip + dx + nc, nc) + (1 - core if other else core)

    def hd(d):
        return pl.ds(pl.multiple_of(d * hl, hl), hl)

    first, second, both = pl.ds(0, H), pl.ds(H, H), pl.ds(0, SC)
    pairs, pairs1, pairs2 = pl.ds(0, H), pl.ds(0, H // 2), pl.ds(H // 2, H // 2)
    right, left, opp, mate = dev(1, 0), dev(-1, 0), dev(2, 0), dev(0, 1)
    right1, left1, opp1 = dev(1, 1), dev(-1, 1), dev(2, 1)

    def same_q(g, part, d):
        r = q_v.at[g, part, hd(d)]
        return r, r

    def msg(kind, g):
        if kind == 'QR':
            src, dst = same_q(g, pairs, me)
            to = right
        elif kind == 'QL':
            src, dst = same_q(g, pairs, me)
            to = left
        elif kind == 'FR':
            src, dst = same_q(g, pairs1, left)
            to = right
        elif kind == 'FL':
            src, dst = same_q(g, pairs2, right)
            to = left
        elif kind == 'ML':
            src, dst = same_q(g, pairs, left)
            to = mate
        elif kind == 'MR':
            src, dst = same_q(g, pairs, right)
            to = mate
        elif kind == 'MO':
            src, dst = same_q(g, pairs, opp)
            to = mate
        elif kind == 'QM':
            src, dst = same_q(g, pairs, me)
            to = mate
        elif kind == 'TR':
            src, dst, to = t_s.at[g], t_l.at[g], right
        elif kind == 'TL':
            src, dst, to = t_s.at[g], t_r.at[g], left
        elif kind == 'S1':
            src, dst, to = z_own.at[g], z_mate.at[g], mate
        elif kind == 'S2':
            src, dst, to = y_s.at[0, g], y_l.at[0, g], right
        elif kind == 'S3':
            src, dst, to = y_s.at[0, g], y_l.at[1, g], right1
        elif kind == 'S4':
            src, dst, to = y_s.at[1, g], y_r.at[0, g], left
        elif kind == 'S5':
            src, dst, to = y_s.at[1, g], y_r.at[1, g], left1
        elif kind == 'MA':
            src, dst, to = o_v.at[g, both, hd(mate)], m_a.at[g], mate
        elif kind == 'MB':
            src, dst, to = o_v.at[g, first, hd(right1)], m_b.at[g], mate
        elif kind == 'MC':
            src, dst, to = o_v.at[g, second, hd(left1)], m_c.at[g], mate
        elif kind == 'HR0':
            src, dst, to = o_v.at[g, first, hd(opp)], h_p.at[0, g], right
        elif kind == 'HR1':
            src, dst, to = o_v.at[g, first, hd(opp1)], h_p.at[1, g], right1
        elif kind == 'HL0':
            src, dst, to = o_v.at[g, second, hd(opp)], h_n.at[0, g], left
        elif kind == 'HL1':
            src, dst, to = o_v.at[g, second, hd(opp1)], h_n.at[1, g], left1
        elif kind == 'DR0':
            src, dst, to = o_v.at[g, second, hd(right)], d_p.at[0, g], right
        elif kind == 'DR1':
            src, dst, to = o_v.at[g, second, hd(right1)], d_p.at[1, g], right1
        elif kind == 'DL0':
            src, dst, to = o_v.at[g, first, hd(left)], d_n.at[0, g], left
        elif kind == 'DL1':
            src, dst, to = o_v.at[g, first, hd(left1)], d_n.at[1, g], left1
        elif kind == 'AR':
            src, dst, to = a_p.at[g], r_p.at[g], right
        else:
            src, dst, to = a_n.at[g], r_n.at[g], left
        i = SEM[kind]
        return pltpu.make_async_remote_copy(
            src_ref=src, dst_ref=dst, send_sem=send.at[i, g], recv_sem=recv.at[i, g],
            device_id={'dcp': to}, device_id_type=pl.DeviceIdType.MESH)

    def start(g, *kinds):
        for k in kinds:
            msg(k, g).start()

    def arrived(g, *kinds):
        for k in kinds:
            msg(k, g).wait_recv()

    def load(g, i):
        slot = lax.rem(g, 2) * SC + i
        return pltpu.make_async_copy(c_hbm.at[g, i], c_v.at[slot], c_sem.at[slot])

    barrier = pltpu.get_barrier_semaphore()
    for d in (mate, right, right1, left, left1):
        pl.semaphore_signal(barrier, inc=1, device_id={'dcp': d}, device_id_type=pl.DeviceIdType.MESH)

    def fetch(g):
        return pltpu.make_async_copy(q_hbm.at[g], q_st.at[g], q_sem.at[g])

    def fetch_start(g, carry):
        fetch(g).start()
        return carry

    lax.fori_loop(0, G, fetch_start, 0)
    lens = pltpu.make_async_copy(len_hbm, len_ref, len_sem)
    lens.start()
    for g in range(min(2, G)):
        for i in range(SC):
            load(g, i).start()
    wrow[...] = jnp.zeros_like(wrow)

    def pack(g):
        fetch(g).wait()
        for p in range(H):
            a, b = q_st[g, 2 * p], q_st[g, 2 * p + 1]
            q_v[g, p, hd(me), :lat] = a[:, :lat]
            q_v[g, p, hd(me), lat:2 * lat] = b[:, :lat]
            q_v[g, p, hd(me), 2 * lat:] = jnp.concatenate([a[:, lat:], b[:, lat:]], axis=1)

    for g in range(min(QD, G)):
        pack(g)
        if g == 0:
            pl.semaphore_wait(barrier, 5)
        start(g, 'QR', 'QL', 'QM')
    lens.wait()

    def attention(g):
        for i in range(SC):
            load(g, i).wait()
        pos = me * sl + lax.broadcasted_iota(jnp.int32, (1, sl), 1)

        def scores(i):
            c = c_v.at[lax.rem(g, 2) * SC + i]
            p, r = divmod(i, 2)
            rope = q_v[g, p, :, 2 * lat + r * ROPE:2 * lat + (r + 1) * ROPE]
            return (jnp.dot(q_v[g, p, :, r * lat:(r + 1) * lat], c[:lat], preferred_element_type=F32)
                    + jnp.dot(rope, c[lat:], preferred_element_type=F32))

        ahead = scores(0)
        for i in range(SC):
            c = c_v.at[lax.rem(g, 2) * SC + i]
            s, ahead = ahead, scores(i + 1) if i + 1 < SC else None
            s = jnp.where(pos < len_ref[g * SC + i], s * SCALE, -jnp.inf)
            m = jnp.max(s, axis=1, keepdims=True)
            m0 = jnp.where(m > -jnp.inf, m, 0.0)
            p = jnp.exp(s - m0)
            l = jnp.sum(p, axis=1, keepdims=True)
            pv = lax.dot_general(p.astype(BF16), c[:lat], NT, preferred_element_type=F32)
            has = l > 0.0
            l1 = jnp.where(has, l, 1.0)
            o_v[g, i] = (pv * (1.0 / l1)).astype(BF16)
            lse_c[i] = jnp.broadcast_to(jnp.where(has, m0 + jnp.log(l1), -jnp.inf), (heads, 128))
        lane = lax.broadcasted_iota(jnp.int32, (2 * hl, 128), 1)
        columns = []
        for i in range(SC):
            block = jnp.zeros((2 * hl, 128), F32)
            for r, steps in enumerate(ROWS):
                c = lax.rem(chip + steps[i // H] + nc, nc)
                block = jnp.where(lane == r, lse_c[i, pl.ds(pl.multiple_of(c * 2 * hl, 2 * hl), 2 * hl)], block)
            columns.append(block)
        rows = jnp.concatenate(columns, axis=0).T
        z_own[g] = rows[:2]
        y_s[0, g] = rows[2:3]
        y_s[1, g] = rows[3:4]

    early = lax.broadcasted_iota(jnp.int32, (1, 128), 1) < 2 * hl * H

    def softmax(ls):
        mx = functools.reduce(jnp.maximum, ls)
        mx = jnp.where(mx > -jnp.inf, mx, 0.0)
        es = [jnp.exp(x - mx) for x in ls]
        z = functools.reduce(jnp.add, es)
        has = z > 0.0
        z1 = jnp.where(has, z, 1.0)
        r = 1.0 / z1
        for k, e in enumerate(es):
            wrow[k:k + 1, :] = e * r
        wt[...] = wrow[...].T
        return jnp.where(has, mx + jnp.log(z1), -jnp.inf)

    def weighted(k, i, o):
        w = wt[pl.ds(pl.multiple_of((2 * i + core) * hl, hl), hl)]
        return w[:, k:k + 1] * o.astype(F32)

    def sums(g):
        arrived(g, 'S1', 'S2', 'S3', 'S4', 'S5')
        t_s[g] = softmax([z_own[g, 0:1], z_mate[g, 0:1]] + [jnp.where(early, y_l[k, g], y_r[k, g]) for k in range(2)])
        start(g, 'TR', 'TL')
        arrived(g, 'HR0', 'HR1', 'HL0', 'HL1', 'MB', 'MC')
        for i0, d, m, h, a in ((0, right, m_b, h_p, a_p), (H, left, m_c, h_n, a_n)):
            for j in range(H):
                i = i0 + j
                a[g, j] = (weighted(0, i, o_v[g, i, hd(d)]) + weighted(1, i, m[g, j])
                           + weighted(2, i, h[0, g, j]) + weighted(3, i, h[1, g, j]))
        start(g, 'AR', 'AL')

    def final(g):
        arrived(g, 'MA', 'TR', 'TL')
        softmax([z_own[g, 1:2], z_mate[g, 1:2]] + [jnp.where(early, y_r[k, g], y_l[k, g]) for k in range(2)]
                + [jnp.where(early, t_l[g], t_r[g])])
        arrived(g, 'DR0', 'DR1', 'DL0', 'DL1', 'AR', 'AL')
        for i in range(SC):
            d, r, j = (d_n, r_p, i) if i < H else (d_p, r_n, i - H)
            out_v[g, i] = (weighted(0, i, o_v[g, i, hd(me)]) + weighted(1, i, m_a[g, i])
                           + weighted(2, i, d[0, g, j]) + weighted(3, i, d[1, g, j])
                           + weighted(4, i, r[g, j])).astype(BF16)

    def stage(t, lag, extra=0):
        g = t - lag
        return g, (g >= 0) & (g < G - extra)

    def step(t, carry):
        a, on = stage(t, 0)

        @pl.when(on)
        def _():
            arrived(a, 'QR', 'QL')
            start(a, 'FR', 'FL', 'ML', 'MR')

        for h in range(QD, G):
            @pl.when(t == OWN_AT.get(h, h - QD))
            def _():
                pack(h)
                start(h, 'QR', 'QL', 'QM')

        b, on = stage(t, 1)

        @pl.when(on)
        def _():
            arrived(b, 'FR', 'FL')
            start(b, 'MO')

        e, on = stage(t, 2 + D2)

        @pl.when(on)
        def _():
            start(e, 'DR0', 'DR1', 'DL0', 'DL1')

        g, on = stage(t, 2)

        @pl.when(on)
        def _():
            arrived(g, 'QM', 'ML', 'MR', 'MO')
            attention(g)
            start(g, 'HR0', 'HR1', 'HL0', 'HL1', 'S1', 'S2', 'S3', 'S4', 'S5', 'MB', 'MC', 'MA')

        @pl.when(stage(t, 2, 2)[1])
        def _():
            for i in range(SC):
                load(t, i).start()

        d, on = stage(t, 2 + D1)

        @pl.when(on)
        def _():
            sums(d)

        return carry

    lax.fori_loop(0, G + 2, step, 0)

    def direct(g, carry):
        start(g, 'DR0', 'DR1', 'DL0', 'DL1')
        return carry

    lax.fori_loop(G - D2, G, direct, 0)

    def rest(g, carry):
        sums(g)
        return carry

    lax.fori_loop(G - D1, G, rest, 0)

    def sent(g):
        for k in KINDS:
            msg(k, g).wait_send()

    def finish(g, carry):
        @pl.when(g >= 1)
        def _():
            sent(g - 1)

        final(g)
        return carry

    lax.fori_loop(0, G, finish, 0)
    sent(G - 1)


def solution(mesh):
    n = mesh.shape['dcp']

    def local(q, cache, lengths):
        b, sl, wd = cache.shape
        hl = q.shape[1]
        heads = hl * n
        lat = wd - ROPE
        G = b // SC
        ct = jnp.swapaxes(cache, 1, 2).reshape(G, SC, wd, sl)
        vmem = pltpu.VMEM
        out = pl.pallas_call(
            functools.partial(kernel, n),
            out_shape=vmem((G, SC, hl, lat), BF16),
            in_specs=[pl.BlockSpec(memory_space=pl.ANY)] * 3,
            out_specs=pl.BlockSpec(memory_space=pltpu.VMEM),
            scratch_shapes=[
                pltpu.SMEM((b,), jnp.int32),
                vmem((G, SC, hl, wd), BF16),
                vmem((G, H, heads, 2 * wd), BF16),
                vmem((2 * SC, wd, sl), BF16),
                vmem((G, SC, heads, lat), BF16),
                vmem((SC, heads, 128), F32),
                vmem((G, 2, 128), F32),
                vmem((G, 2, 128), F32),
                vmem((2, G, 1, 128), F32),
                vmem((2, G, 1, 128), F32),
                vmem((2, G, 1, 128), F32),
                vmem((G, 1, 128), F32),
                vmem((G, 1, 128), F32),
                vmem((G, 1, 128), F32),
                vmem((128, 128), F32),
                vmem((128, 128), F32),
                vmem((G, SC, hl, lat), BF16),
                vmem((G, H, hl, lat), BF16),
                vmem((G, H, hl, lat), BF16),
                vmem((2, G, H, hl, lat), BF16),
                vmem((2, G, H, hl, lat), BF16),
                vmem((2, G, H, hl, lat), BF16),
                vmem((2, G, H, hl, lat), BF16),
                vmem((G, H, hl, lat), F32),
                vmem((G, H, hl, lat), F32),
                vmem((G, H, hl, lat), F32),
                vmem((G, H, hl, lat), F32),
                pltpu.SemaphoreType.DMA((len(KINDS), G)),
                pltpu.SemaphoreType.DMA((len(KINDS), G)),
                pltpu.SemaphoreType.DMA,
                pltpu.SemaphoreType.DMA((G,)),
                pltpu.SemaphoreType.DMA((2 * SC,)),
            ],
            compiler_params=pltpu.CompilerParams(
                collective_id=0, has_side_effects=True, vmem_limit_bytes=56 * 2 ** 20),
        )(lengths, q.reshape(G, SC, hl, wd), ct)
        return out.reshape(b, hl, lat)

    return jax.shard_map(local, mesh=mesh, in_specs=(P('dp', 'dcp', None), P('dp', 'dcp', None), P('dp')),
                         out_specs=P('dp', 'dcp', None), check_vma=False)
```

```python
import functools

import jax
import jax.numpy as jnp
from jax import lax
from jax.experimental import pallas as pl
from jax.experimental.pallas import tpu as pltpu
from jax.sharding import PartitionSpec as P

ROPE = 64
SCALE = 192 ** -0.5
F32 = jnp.float32
BF16 = jnp.bfloat16
NT = (((1,), (1,)), ((), ()))

SC = 4
H = SC // 2
OWN_AT = {6: 2, 7: 3}
QD = 3
D1, D2 = 2, 2

ROWS = ((1, -1), (0, 0), (2, 1), (-1, 2))

ARRIVE = (('QR', 'QL'), ('FR', 'FL'), ('QM', 'ML', 'MR', 'MO'), ('S1', 'S2', 'S3', 'S4', 'S5'),
          ('HR0', 'HR1', 'HL0', 'HL1', 'MB', 'MC'), ('TR', 'TL'),
          ('MA', 'DR0', 'DR1', 'DL0', 'DL1', 'AR', 'AL'))
NEAR, FAR, QUERIES, LSE, HOPS, SUM_LSE, LAST = range(len(ARRIVE))
LEAVE = (('QR', 'QL', 'FR', 'FL', 'QM', 'ML', 'MR', 'MO'),
         ('HR0', 'HR1', 'HL0', 'HL1', 'MA', 'MB', 'MC', 'DR0', 'DR1', 'DL0', 'DL1', 'AR', 'AL'),
         ('S1', 'S2', 'S3', 'S4', 'S5', 'TR', 'TL'))
ARRIVE_SEM = {k: c for c, ks in enumerate(ARRIVE) for k in ks}
LEAVE_SEM = {k: c for c, ks in enumerate(LEAVE) for k in ks}


def kernel(n, len_hbm, q_hbm, c_hbm, out_v,
           len_ref, q_st, q_v, c_v, o_v, lse_c, z_own, z_mate, y_s, y_l, y_r, t_s, t_l, t_r, wrow, wt, m_a, m_b, m_c, h_p, h_n, d_p, d_n, a_p, a_n, r_p, r_n,
           send, recv, len_sem, q_sem, c_sem):
    G = q_v.shape[0]
    lat = o_v.shape[3]
    heads = o_v.shape[2]
    hl = heads // n
    sl = c_v.shape[2]
    nc = n // 2
    me = lax.axis_index('dcp')
    chip = lax.div(me, 2)
    core = lax.rem(me, 2)

    def dev(dx, other):
        return 2 * lax.rem(chip + dx + nc, nc) + (1 - core if other else core)

    def hd(d):
        return pl.ds(pl.multiple_of(d * hl, hl), hl)

    first, second, both = pl.ds(0, H), pl.ds(H, H), pl.ds(0, SC)
    pairs, pairs1, pairs2 = pl.ds(0, H), pl.ds(0, H // 2), pl.ds(H // 2, H // 2)
    right, left, opp, mate = dev(1, 0), dev(-1, 0), dev(2, 0), dev(0, 1)
    right1, left1, opp1 = dev(1, 1), dev(-1, 1), dev(2, 1)

    def same_q(g, part, d):
        r = q_v.at[g, part, hd(d)]
        return r, r

    def msg(kind, g):
        if kind == 'QR':
            src, dst = same_q(g, pairs, me)
            to = right
        elif kind == 'QL':
            src, dst = same_q(g, pairs, me)
            to = left
        elif kind == 'FR':
            src, dst = same_q(g, pairs1, left)
            to = right
        elif kind == 'FL':
            src, dst = same_q(g, pairs2, right)
            to = left
        elif kind == 'ML':
            src, dst = same_q(g, pairs, left)
            to = mate
        elif kind == 'MR':
            src, dst = same_q(g, pairs, right)
            to = mate
        elif kind == 'MO':
            src, dst = same_q(g, pairs, opp)
            to = mate
        elif kind == 'QM':
            src, dst = same_q(g, pairs, me)
            to = mate
        elif kind == 'TR':
            src, dst, to = t_s.at[g], t_l.at[g], right
        elif kind == 'TL':
            src, dst, to = t_s.at[g], t_r.at[g], left
        elif kind == 'S1':
            src, dst, to = z_own.at[g], z_mate.at[g], mate
        elif kind == 'S2':
            src, dst, to = y_s.at[0, g], y_l.at[0, g], right
        elif kind == 'S3':
            src, dst, to = y_s.at[0, g], y_l.at[1, g], right1
        elif kind == 'S4':
            src, dst, to = y_s.at[1, g], y_r.at[0, g], left
        elif kind == 'S5':
            src, dst, to = y_s.at[1, g], y_r.at[1, g], left1
        elif kind == 'MA':
            src, dst, to = o_v.at[g, both, hd(mate)], m_a.at[g], mate
        elif kind == 'MB':
            src, dst, to = o_v.at[g, first, hd(right1)], m_b.at[g], mate
        elif kind == 'MC':
            src, dst, to = o_v.at[g, second, hd(left1)], m_c.at[g], mate
        elif kind == 'HR0':
            src, dst, to = o_v.at[g, first, hd(opp)], h_p.at[0, g], right
        elif kind == 'HR1':
            src, dst, to = o_v.at[g, first, hd(opp1)], h_p.at[1, g], right1
        elif kind == 'HL0':
            src, dst, to = o_v.at[g, second, hd(opp)], h_n.at[0, g], left
        elif kind == 'HL1':
            src, dst, to = o_v.at[g, second, hd(opp1)], h_n.at[1, g], left1
        elif kind == 'DR0':
            src, dst, to = o_v.at[g, second, hd(right)], d_p.at[0, g], right
        elif kind == 'DR1':
            src, dst, to = o_v.at[g, second, hd(right1)], d_p.at[1, g], right1
        elif kind == 'DL0':
            src, dst, to = o_v.at[g, first, hd(left)], d_n.at[0, g], left
        elif kind == 'DL1':
            src, dst, to = o_v.at[g, first, hd(left1)], d_n.at[1, g], left1
        elif kind == 'AR':
            src, dst, to = a_p.at[g], r_p.at[g], right
        else:
            src, dst, to = a_n.at[g], r_n.at[g], left
        return pltpu.make_async_remote_copy(
            src_ref=src, dst_ref=dst, send_sem=send.at[LEAVE_SEM[kind], g], recv_sem=recv.at[ARRIVE_SEM[kind], g],
            device_id={'dcp': to}, device_id_type=pl.DeviceIdType.MESH)

    def start(g, *kinds):
        for k in kinds:
            msg(k, g).start()

    arrive_bytes = (q_v.at[0, pairs, 0:2 * hl], q_v.at[0, pairs, 0:hl], q_v.at[0, pairs, 0:4 * hl], z_own.at[0:3],
                    o_v.at[0, 0:3, 0:4 * hl], z_own.at[0], o_v.at[0, both, 0:5 * hl])
    leave_bytes = (q_v.at[0, pairs, 0:7 * hl], o_v.at[0], z_own.at[0:4])

    def pending(ref, g, c):
        return pltpu.make_async_remote_copy(
            src_ref=ref, dst_ref=ref, send_sem=send.at[c % len(LEAVE), g], recv_sem=recv.at[c, g],
            device_id={'dcp': mate}, device_id_type=pl.DeviceIdType.MESH)

    def arrived(g, c):
        pending(arrive_bytes[c], g, c).wait_recv()

    def sent(g):
        for c, ref in enumerate(leave_bytes):
            pending(ref, g, c).wait_send()

    def load(g, i):
        slot = lax.rem(g, 2) * SC + i
        return pltpu.make_async_copy(c_hbm.at[g, i], c_v.at[slot], c_sem.at[slot])

    barrier = pltpu.get_barrier_semaphore()
    for d in (mate, right, right1, left, left1):
        pl.semaphore_signal(barrier, inc=1, device_id={'dcp': d}, device_id_type=pl.DeviceIdType.MESH)

    def fetch(g):
        return pltpu.make_async_copy(q_hbm.at[g], q_st.at[g], q_sem.at[g])

    def fetch_start(g, carry):
        fetch(g).start()
        return carry

    lax.fori_loop(0, G, fetch_start, 0)
    lens = pltpu.make_async_copy(len_hbm, len_ref, len_sem)
    lens.start()
    for g in range(min(2, G)):
        for i in range(SC):
            load(g, i).start()
    wrow[...] = jnp.zeros_like(wrow)

    def pack(g):
        fetch(g).wait()
        for p in range(H):
            a, b = q_st[g, 2 * p], q_st[g, 2 * p + 1]
            q_v[g, p, hd(me), :lat] = a[:, :lat]
            q_v[g, p, hd(me), lat:2 * lat] = b[:, :lat]
            q_v[g, p, hd(me), 2 * lat:] = jnp.concatenate([a[:, lat:], b[:, lat:]], axis=1)

    for g in range(min(QD, G)):
        pack(g)
        if g == 0:
            pl.semaphore_wait(barrier, 5)
        start(g, 'QR', 'QL', 'QM')
    lens.wait()

    def attention(g):
        for i in range(SC):
            load(g, i).wait()
        pos = me * sl + lax.broadcasted_iota(jnp.int32, (1, sl), 1)

        def scores(i):
            c = c_v.at[lax.rem(g, 2) * SC + i]
            p, r = divmod(i, 2)
            rope = q_v[g, p, :, 2 * lat + r * ROPE:2 * lat + (r + 1) * ROPE]
            return (jnp.dot(q_v[g, p, :, r * lat:(r + 1) * lat], c[:lat], preferred_element_type=F32)
                    + jnp.dot(rope, c[lat:], preferred_element_type=F32))

        ahead = scores(0)
        for i in range(SC):
            c = c_v.at[lax.rem(g, 2) * SC + i]
            s, ahead = ahead, scores(i + 1) if i + 1 < SC else None
            s = jnp.where(pos < len_ref[g * SC + i], s * SCALE, -jnp.inf)
            m = jnp.max(s, axis=1, keepdims=True)
            m0 = jnp.where(m > -jnp.inf, m, 0.0)
            p = jnp.exp(s - m0)
            l = jnp.sum(p, axis=1, keepdims=True)
            pv = lax.dot_general(p.astype(BF16), c[:lat], NT, preferred_element_type=F32)
            has = l > 0.0
            l1 = jnp.where(has, l, 1.0)
            o_v[g, i] = (pv * (1.0 / l1)).astype(BF16)
            lse_c[i] = jnp.broadcast_to(jnp.where(has, m0 + jnp.log(l1), -jnp.inf), (heads, 128))
        lane = lax.broadcasted_iota(jnp.int32, (2 * hl, 128), 1)
        columns = []
        for i in range(SC):
            block = jnp.zeros((2 * hl, 128), F32)
            for r, steps in enumerate(ROWS):
                c = lax.rem(chip + steps[i // H] + nc, nc)
                block = jnp.where(lane == r, lse_c[i, pl.ds(pl.multiple_of(c * 2 * hl, 2 * hl), 2 * hl)], block)
            columns.append(block)
        rows = jnp.concatenate(columns, axis=0).T
        z_own[g] = rows[:2]
        y_s[0, g] = rows[2:3]
        y_s[1, g] = rows[3:4]

    early = lax.broadcasted_iota(jnp.int32, (1, 128), 1) < 2 * hl * H

    def softmax(ls):
        mx = functools.reduce(jnp.maximum, ls)
        mx = jnp.where(mx > -jnp.inf, mx, 0.0)
        es = [jnp.exp(x - mx) for x in ls]
        z = functools.reduce(jnp.add, es)
        has = z > 0.0
        z1 = jnp.where(has, z, 1.0)
        r = 1.0 / z1
        for k, e in enumerate(es):
            wrow[k:k + 1, :] = e * r
        wt[...] = wrow[...].T
        return jnp.where(has, mx + jnp.log(z1), -jnp.inf)

    def weighted(k, i, o):
        w = wt[pl.ds(pl.multiple_of((2 * i + core) * hl, hl), hl)]
        return w[:, k:k + 1] * o.astype(F32)

    def sums(g):
        arrived(g, LSE)
        t_s[g] = softmax([z_own[g, 0:1], z_mate[g, 0:1]] + [jnp.where(early, y_l[k, g], y_r[k, g]) for k in range(2)])
        start(g, 'TR', 'TL')
        arrived(g, HOPS)
        for i0, d, m, h, a in ((0, right, m_b, h_p, a_p), (H, left, m_c, h_n, a_n)):
            for j in range(H):
                i = i0 + j
                a[g, j] = (weighted(0, i, o_v[g, i, hd(d)]) + weighted(1, i, m[g, j])
                           + weighted(2, i, h[0, g, j]) + weighted(3, i, h[1, g, j]))
        start(g, 'AR', 'AL')

    def final(g):
        arrived(g, SUM_LSE)
        softmax([z_own[g, 1:2], z_mate[g, 1:2]] + [jnp.where(early, y_r[k, g], y_l[k, g]) for k in range(2)]
                + [jnp.where(early, t_l[g], t_r[g])])
        arrived(g, LAST)
        for i in range(SC):
            d, r, j = (d_n, r_p, i) if i < H else (d_p, r_n, i - H)
            out_v[g, i] = (weighted(0, i, o_v[g, i, hd(me)]) + weighted(1, i, m_a[g, i])
                           + weighted(2, i, d[0, g, j]) + weighted(3, i, d[1, g, j])
                           + weighted(4, i, r[g, j])).astype(BF16)

    def stage(t, lag, extra=0):
        g = t - lag
        return g, (g >= 0) & (g < G - extra)

    def step(t, carry):
        a, on = stage(t, 0)

        @pl.when(on)
        def _():
            arrived(a, NEAR)
            start(a, 'FR', 'FL', 'ML', 'MR')

        for h in range(QD, G):
            @pl.when(t == OWN_AT.get(h, h - QD))
            def _():
                pack(h)
                start(h, 'QR', 'QL', 'QM')

        b, on = stage(t, 1)

        @pl.when(on)
        def _():
            arrived(b, FAR)
            start(b, 'MO')

        e, on = stage(t, 2 + D2)

        @pl.when(on)
        def _():
            start(e, 'DR0', 'DR1', 'DL0', 'DL1')

        g, on = stage(t, 2)

        @pl.when(on)
        def _():
            arrived(g, QUERIES)
            attention(g)
            start(g, 'HR0', 'HR1', 'HL0', 'HL1', 'S1', 'S2', 'S3', 'S4', 'S5', 'MB', 'MC', 'MA')

        @pl.when(stage(t, 2, 2)[1])
        def _():
            for i in range(SC):
                load(t, i).start()

        d, on = stage(t, 2 + D1)

        @pl.when(on)
        def _():
            sums(d)

        return carry

    lax.fori_loop(0, G + 2, step, 0)

    def direct(g, carry):
        start(g, 'DR0', 'DR1', 'DL0', 'DL1')
        return carry

    lax.fori_loop(G - D2, G, direct, 0)

    def rest(g, carry):
        sums(g)
        return carry

    lax.fori_loop(G - D1, G, rest, 0)

    def finish(g, carry):
        @pl.when(g >= 1)
        def _():
            sent(g - 1)

        final(g)
        return carry

    lax.fori_loop(0, G, finish, 0)
    sent(G - 1)


def solution(mesh):
    n = mesh.shape['dcp']

    def local(q, cache, lengths):
        b, sl, wd = cache.shape
        hl = q.shape[1]
        heads = hl * n
        lat = wd - ROPE
        G = b // SC
        ct = jnp.swapaxes(cache, 1, 2).reshape(G, SC, wd, sl)
        vmem = pltpu.VMEM
        out = pl.pallas_call(
            functools.partial(kernel, n),
            out_shape=vmem((G, SC, hl, lat), BF16),
            in_specs=[pl.BlockSpec(memory_space=pl.ANY)] * 3,
            out_specs=pl.BlockSpec(memory_space=pltpu.VMEM),
            scratch_shapes=[
                pltpu.SMEM((b,), jnp.int32),
                vmem((G, SC, hl, wd), BF16),
                vmem((G, H, heads, 2 * wd), BF16),
                vmem((2 * SC, wd, sl), BF16),
                vmem((G, SC, heads, lat), BF16),
                vmem((SC, heads, 128), F32),
                vmem((G, 2, 128), F32),
                vmem((G, 2, 128), F32),
                vmem((2, G, 1, 128), F32),
                vmem((2, G, 1, 128), F32),
                vmem((2, G, 1, 128), F32),
                vmem((G, 1, 128), F32),
                vmem((G, 1, 128), F32),
                vmem((G, 1, 128), F32),
                vmem((128, 128), F32),
                vmem((128, 128), F32),
                vmem((G, SC, hl, lat), BF16),
                vmem((G, H, hl, lat), BF16),
                vmem((G, H, hl, lat), BF16),
                vmem((2, G, H, hl, lat), BF16),
                vmem((2, G, H, hl, lat), BF16),
                vmem((2, G, H, hl, lat), BF16),
                vmem((2, G, H, hl, lat), BF16),
                vmem((G, H, hl, lat), F32),
                vmem((G, H, hl, lat), F32),
                vmem((G, H, hl, lat), F32),
                vmem((G, H, hl, lat), F32),
                pltpu.SemaphoreType.DMA((len(LEAVE), G)),
                pltpu.SemaphoreType.DMA((len(ARRIVE), G)),
                pltpu.SemaphoreType.DMA,
                pltpu.SemaphoreType.DMA((G,)),
                pltpu.SemaphoreType.DMA((2 * SC,)),
            ],
            compiler_params=pltpu.CompilerParams(
                collective_id=0, has_side_effects=True, vmem_limit_bytes=56 * 2 ** 20),
        )(lengths, q.reshape(G, SC, hl, wd), ct)
        return out.reshape(b, hl, lat)

    return jax.shard_map(local, mesh=mesh, in_specs=(P('dp', 'dcp', None), P('dp', 'dcp', None), P('dp')),
                         out_specs=P('dp', 'dcp', None), check_vma=False)
```

```python
import functools

import jax
import jax.numpy as jnp
from jax import lax
from jax.experimental import pallas as pl
from jax.experimental.pallas import tpu as pltpu
from jax.sharding import PartitionSpec as P

ROPE = 64
SCALE = 192 ** -0.5
F32 = jnp.float32
BF16 = jnp.bfloat16
NT = (((1,), (1,)), ((), ()))

SC = 4
H = SC // 2
OWN_AT = {6: 2, 7: 3}
QD = 3
D1, D2 = 2, 2

ROWS = ((1, -1), (0, 0), (2, 1), (-1, 2))

ARRIVE = (('QR', 'QL'), ('FR', 'FL'), ('QM', 'ML', 'MR', 'MO'), ('S1', 'S2', 'S3', 'S4', 'S5'),
          ('HR0', 'HR1', 'HL0', 'HL1', 'MB', 'MC'), ('TR', 'TL'),
          ('MA', 'DR0', 'DR1', 'DL0', 'DL1', 'AR', 'AL'))
NEAR, FAR, QUERIES, LSE, HOPS, SUM_LSE, LAST = range(len(ARRIVE))
LEAVE = (('QR', 'QL', 'FR', 'FL', 'QM', 'ML', 'MR', 'MO'),
         ('HR0', 'HR1', 'HL0', 'HL1', 'MA', 'MB', 'MC', 'DR0', 'DR1', 'DL0', 'DL1', 'AR', 'AL'),
         ('S1', 'S2', 'S3', 'S4', 'S5', 'TR', 'TL'))
ARRIVE_SEM = {k: c for c, ks in enumerate(ARRIVE) for k in ks}
LEAVE_SEM = {k: c for c, ks in enumerate(LEAVE) for k in ks}


def kernel(n, len_hbm, q_hbm, c_hbm, out_v,
           len_ref, q_st, q_v, c_v, o_v, lse_c, z_own, z_mate, y_s, y_l, y_r, t_s, t_l, t_r, wrow, wt, m_a, m_b, m_c, h_p, h_n, d_p, d_n, a_p, a_n, r_p, r_n,
           send, recv, len_sem, q_sem, c_sem):
    G = q_v.shape[0]
    lat = o_v.shape[3]
    heads = o_v.shape[2]
    hl = heads // n
    sl = c_v.shape[3]
    nc = n // 2
    me = lax.axis_index('dcp')
    chip = lax.div(me, 2)
    core = lax.rem(me, 2)

    def dev(dx, other):
        return 2 * lax.rem(chip + dx + nc, nc) + (1 - core if other else core)

    def hd(d):
        return pl.ds(pl.multiple_of(d * hl, hl), hl)

    first, second, both = pl.ds(0, H), pl.ds(H, H), pl.ds(0, SC)
    pairs, pairs1, pairs2 = pl.ds(0, H), pl.ds(0, H // 2), pl.ds(H // 2, H // 2)
    right, left, opp, mate = dev(1, 0), dev(-1, 0), dev(2, 0), dev(0, 1)
    right1, left1, opp1 = dev(1, 1), dev(-1, 1), dev(2, 1)

    def same_q(g, part, d):
        r = q_v.at[g, part, hd(d)]
        return r, r

    def msg(kind, g):
        if kind == 'QR':
            src, dst = same_q(g, pairs, me)
            to = right
        elif kind == 'QL':
            src, dst = same_q(g, pairs, me)
            to = left
        elif kind == 'FR':
            src, dst = same_q(g, pairs1, left)
            to = right
        elif kind == 'FL':
            src, dst = same_q(g, pairs2, right)
            to = left
        elif kind == 'ML':
            src, dst = same_q(g, pairs, left)
            to = mate
        elif kind == 'MR':
            src, dst = same_q(g, pairs, right)
            to = mate
        elif kind == 'MO':
            src, dst = same_q(g, pairs, opp)
            to = mate
        elif kind == 'QM':
            src, dst = same_q(g, pairs, me)
            to = mate
        elif kind == 'TR':
            src, dst, to = t_s.at[g], t_l.at[g], right
        elif kind == 'TL':
            src, dst, to = t_s.at[g], t_r.at[g], left
        elif kind == 'S1':
            src, dst, to = z_own.at[g], z_mate.at[g], mate
        elif kind == 'S2':
            src, dst, to = y_s.at[0, g], y_l.at[0, g], right
        elif kind == 'S3':
            src, dst, to = y_s.at[0, g], y_l.at[1, g], right1
        elif kind == 'S4':
            src, dst, to = y_s.at[1, g], y_r.at[0, g], left
        elif kind == 'S5':
            src, dst, to = y_s.at[1, g], y_r.at[1, g], left1
        elif kind == 'MA':
            src, dst, to = o_v.at[g, both, hd(mate)], m_a.at[g], mate
        elif kind == 'MB':
            src, dst, to = o_v.at[g, first, hd(right1)], m_b.at[g], mate
        elif kind == 'MC':
            src, dst, to = o_v.at[g, second, hd(left1)], m_c.at[g], mate
        elif kind == 'HR0':
            src, dst, to = o_v.at[g, first, hd(opp)], h_p.at[0, g], right
        elif kind == 'HR1':
            src, dst, to = o_v.at[g, first, hd(opp1)], h_p.at[1, g], right1
        elif kind == 'HL0':
            src, dst, to = o_v.at[g, second, hd(opp)], h_n.at[0, g], left
        elif kind == 'HL1':
            src, dst, to = o_v.at[g, second, hd(opp1)], h_n.at[1, g], left1
        elif kind == 'DR0':
            src, dst, to = o_v.at[g, second, hd(right)], d_p.at[0, g], right
        elif kind == 'DR1':
            src, dst, to = o_v.at[g, second, hd(right1)], d_p.at[1, g], right1
        elif kind == 'DL0':
            src, dst, to = o_v.at[g, first, hd(left)], d_n.at[0, g], left
        elif kind == 'DL1':
            src, dst, to = o_v.at[g, first, hd(left1)], d_n.at[1, g], left1
        elif kind == 'AR':
            src, dst, to = a_p.at[g], r_p.at[g], right
        else:
            src, dst, to = a_n.at[g], r_n.at[g], left
        return pltpu.make_async_remote_copy(
            src_ref=src, dst_ref=dst, send_sem=send.at[LEAVE_SEM[kind]], recv_sem=recv.at[ARRIVE_SEM[kind], g],
            device_id={'dcp': to}, device_id_type=pl.DeviceIdType.MESH)

    def start(g, *kinds):
        for k in kinds:
            msg(k, g).start()

    arrive_bytes = (q_v.at[0, pairs, 0:2 * hl], q_v.at[0, pairs, 0:hl], q_v.at[0, pairs, 0:4 * hl], z_own.at[0:3],
                    o_v.at[0, 0:3, 0:4 * hl], z_own.at[0], o_v.at[0, both, 0:5 * hl])
    leave_bytes = (q_v.at[:, :, 0:7 * hl], o_v, lse_c.at[0, 0:8 * G])

    def pending(ref, g, c):
        return pltpu.make_async_remote_copy(
            src_ref=ref, dst_ref=ref, send_sem=send.at[c % len(LEAVE)], recv_sem=recv.at[c, g],
            device_id={'dcp': mate}, device_id_type=pl.DeviceIdType.MESH)

    def arrived(g, c):
        pending(arrive_bytes[c], g, c).wait_recv()

    def load(g):
        slot = lax.rem(g, 2)
        return pltpu.make_async_copy(c_hbm.at[g], c_v.at[slot], c_sem.at[slot])

    barrier = pltpu.get_barrier_semaphore()
    for d in (mate, right, right1, left, left1):
        pl.semaphore_signal(barrier, inc=1, device_id={'dcp': d}, device_id_type=pl.DeviceIdType.MESH)

    def fetch(k):
        part = pl.ds(0, 1) if k == 0 else pl.ds(1, G - 1)
        return pltpu.make_async_copy(q_hbm.at[part], q_st.at[part], q_sem.at[k])

    fetch(0).start()
    fetch(1).start()
    lens = pltpu.make_async_copy(len_hbm, len_ref, len_sem)
    lens.start()
    for g in range(min(2, G)):
        load(g).start()
    wrow[...] = jnp.zeros_like(wrow)

    def pack(g):
        for p in range(H):
            a, b = q_st[g, 2 * p], q_st[g, 2 * p + 1]
            q_v[g, p, hd(me), :lat] = a[:, :lat]
            q_v[g, p, hd(me), lat:2 * lat] = b[:, :lat]
            q_v[g, p, hd(me), 2 * lat:] = jnp.concatenate([a[:, lat:], b[:, lat:]], axis=1)

    for g in range(min(QD, G)):
        if g < 2:
            fetch(g).wait()
        pack(g)
        if g == 0:
            pl.semaphore_wait(barrier, 5)
        start(g, 'QR', 'QL', 'QM')
    lens.wait()

    def attention(g):
        load(g).wait()
        pos = me * sl + lax.broadcasted_iota(jnp.int32, (1, sl), 1)

        def scores(i):
            c = c_v.at[lax.rem(g, 2), i]
            p, r = divmod(i, 2)
            rope = q_v[g, p, :, 2 * lat + r * ROPE:2 * lat + (r + 1) * ROPE]
            return (jnp.dot(q_v[g, p, :, r * lat:(r + 1) * lat], c[:lat], preferred_element_type=F32)
                    + jnp.dot(rope, c[lat:], preferred_element_type=F32))

        ahead = scores(0)
        for i in range(SC):
            c = c_v.at[lax.rem(g, 2), i]
            s, ahead = ahead, scores(i + 1) if i + 1 < SC else None
            s = jnp.where(pos < len_ref[g * SC + i], s * SCALE, -jnp.inf)
            m = jnp.max(s, axis=1, keepdims=True)
            m0 = jnp.where(m > -jnp.inf, m, 0.0)
            p = jnp.exp(s - m0)
            l = jnp.sum(p, axis=1, keepdims=True)
            pv = lax.dot_general(p.astype(BF16), c[:lat], NT, preferred_element_type=F32)
            has = l > 0.0
            l1 = jnp.where(has, l, 1.0)
            o_v[g, i] = (pv * (1.0 / l1)).astype(BF16)
            lse_c[i] = jnp.broadcast_to(jnp.where(has, m0 + jnp.log(l1), -jnp.inf), (heads, 128))
        lane = lax.broadcasted_iota(jnp.int32, (2 * hl, 128), 1)
        columns = []
        for i in range(SC):
            block = jnp.zeros((2 * hl, 128), F32)
            for r, steps in enumerate(ROWS):
                c = lax.rem(chip + steps[i // H] + nc, nc)
                block = jnp.where(lane == r, lse_c[i, pl.ds(pl.multiple_of(c * 2 * hl, 2 * hl), 2 * hl)], block)
            columns.append(block)
        rows = jnp.concatenate(columns, axis=0).T
        z_own[g] = rows[:2]
        y_s[0, g] = rows[2:3]
        y_s[1, g] = rows[3:4]

    early = lax.broadcasted_iota(jnp.int32, (1, 128), 1) < 2 * hl * H

    def softmax(ls):
        mx = functools.reduce(jnp.maximum, ls)
        mx = jnp.where(mx > -jnp.inf, mx, 0.0)
        es = [jnp.exp(x - mx) for x in ls]
        z = functools.reduce(jnp.add, es)
        has = z > 0.0
        z1 = jnp.where(has, z, 1.0)
        r = 1.0 / z1
        for k, e in enumerate(es):
            wrow[k:k + 1, :] = e * r
        wt[...] = wrow[...].T
        return jnp.where(has, mx + jnp.log(z1), -jnp.inf)

    def weighted(k, i, o):
        w = wt[pl.ds(pl.multiple_of((2 * i + core) * hl, hl), hl)]
        return w[:, k:k + 1] * o.astype(F32)

    def sums(g):
        arrived(g, LSE)
        t_s[g] = softmax([z_own[g, 0:1], z_mate[g, 0:1]] + [jnp.where(early, y_l[k, g], y_r[k, g]) for k in range(2)])
        start(g, 'TR', 'TL')
        arrived(g, HOPS)
        for i0, d, m, h, a in ((0, right, m_b, h_p, a_p), (H, left, m_c, h_n, a_n)):
            for j in range(H):
                i = i0 + j
                a[g, j] = (weighted(0, i, o_v[g, i, hd(d)]) + weighted(1, i, m[g, j])
                           + weighted(2, i, h[0, g, j]) + weighted(3, i, h[1, g, j]))
        start(g, 'AR', 'AL')

    def final(g):
        arrived(g, SUM_LSE)
        softmax([z_own[g, 1:2], z_mate[g, 1:2]] + [jnp.where(early, y_r[k, g], y_l[k, g]) for k in range(2)]
                + [jnp.where(early, t_l[g], t_r[g])])
        arrived(g, LAST)
        for i in range(SC):
            d, r, j = (d_n, r_p, i) if i < H else (d_p, r_n, i - H)
            out_v[g, i] = (weighted(0, i, o_v[g, i, hd(me)]) + weighted(1, i, m_a[g, i])
                           + weighted(2, i, d[0, g, j]) + weighted(3, i, d[1, g, j])
                           + weighted(4, i, r[g, j])).astype(BF16)

    def stage(t, lag, extra=0):
        g = t - lag
        return g, (g >= 0) & (g < G - extra)

    def step(t, carry):
        a, on = stage(t, 0)

        @pl.when(on)
        def _():
            arrived(a, NEAR)
            start(a, 'FR', 'FL', 'ML', 'MR')

        for h in range(QD, G):
            @pl.when(t == OWN_AT.get(h, h - QD))
            def _():
                pack(h)
                start(h, 'QR', 'QL', 'QM')

        b, on = stage(t, 1)

        @pl.when(on)
        def _():
            arrived(b, FAR)
            start(b, 'MO')

        e, on = stage(t, 2 + D2)

        @pl.when(on)
        def _():
            start(e, 'DR0', 'DR1', 'DL0', 'DL1')

        g, on = stage(t, 2)

        @pl.when(on)
        def _():
            arrived(g, QUERIES)
            attention(g)
            start(g, 'HR0', 'HR1', 'HL0', 'HL1', 'S1', 'S2', 'S3', 'S4', 'S5', 'MB', 'MC', 'MA')

        @pl.when(stage(t, 2, 2)[1])
        def _():
            load(t).start()

        d, on = stage(t, 2 + D1)

        @pl.when(on)
        def _():
            sums(d)

        return carry

    lax.fori_loop(0, G + 2, step, 0)

    def direct(g, carry):
        start(g, 'DR0', 'DR1', 'DL0', 'DL1')
        return carry

    lax.fori_loop(G - D2, G, direct, 0)

    def rest(g, carry):
        sums(g)
        return carry

    lax.fori_loop(G - D1, G, rest, 0)

    def finish(g, carry):
        final(g)
        return carry

    lax.fori_loop(0, G, finish, 0)
    for c, ref in enumerate(leave_bytes):
        pending(ref, 0, c).wait_send()


def solution(mesh):
    n = mesh.shape['dcp']

    def local(q, cache, lengths):
        b, sl, wd = cache.shape
        hl = q.shape[1]
        heads = hl * n
        lat = wd - ROPE
        G = b // SC
        ct = jnp.swapaxes(cache, 1, 2).reshape(G, SC, wd, sl)
        vmem = pltpu.VMEM
        out = pl.pallas_call(
            functools.partial(kernel, n),
            out_shape=vmem((G, SC, hl, lat), BF16),
            in_specs=[pl.BlockSpec(memory_space=pl.ANY)] * 3,
            out_specs=pl.BlockSpec(memory_space=pltpu.VMEM),
            scratch_shapes=[
                pltpu.SMEM((b,), jnp.int32),
                vmem((G, SC, hl, wd), BF16),
                vmem((G, H, heads, 2 * wd), BF16),
                vmem((2, SC, wd, sl), BF16),
                vmem((G, SC, heads, lat), BF16),
                vmem((SC, heads, 128), F32),
                vmem((G, 2, 128), F32),
                vmem((G, 2, 128), F32),
                vmem((2, G, 1, 128), F32),
                vmem((2, G, 1, 128), F32),
                vmem((2, G, 1, 128), F32),
                vmem((G, 1, 128), F32),
                vmem((G, 1, 128), F32),
                vmem((G, 1, 128), F32),
                vmem((128, 128), F32),
                vmem((128, 128), F32),
                vmem((G, SC, hl, lat), BF16),
                vmem((G, H, hl, lat), BF16),
                vmem((G, H, hl, lat), BF16),
                vmem((2, G, H, hl, lat), BF16),
                vmem((2, G, H, hl, lat), BF16),
                vmem((2, G, H, hl, lat), BF16),
                vmem((2, G, H, hl, lat), BF16),
                vmem((G, H, hl, lat), F32),
                vmem((G, H, hl, lat), F32),
                vmem((G, H, hl, lat), F32),
                vmem((G, H, hl, lat), F32),
                pltpu.SemaphoreType.DMA((len(LEAVE),)),
                pltpu.SemaphoreType.DMA((len(ARRIVE), G)),
                pltpu.SemaphoreType.DMA,
                pltpu.SemaphoreType.DMA((2,)),
                pltpu.SemaphoreType.DMA((2,)),
            ],
            compiler_params=pltpu.CompilerParams(
                collective_id=0, has_side_effects=True, vmem_limit_bytes=56 * 2 ** 20),
        )(lengths, q.reshape(G, SC, hl, wd), ct)
        return out.reshape(b, hl, lat)

    return jax.shard_map(local, mesh=mesh, in_specs=(P('dp', 'dcp', None), P('dp', 'dcp', None), P('dp')),
                         out_specs=P('dp', 'dcp', None), check_vma=False)
```

```python
import functools

import jax
import jax.numpy as jnp
from jax import lax
from jax.experimental import pallas as pl
from jax.experimental.pallas import tpu as pltpu
from jax.sharding import PartitionSpec as P

ROPE = 64
SCALE = 192 ** -0.5
F32 = jnp.float32
BF16 = jnp.bfloat16
NT = (((1,), (1,)), ((), ()))

SC = 4
H = SC // 2
OWN_AT = {6: 2, 7: 3}
QD = 3
D1, D2 = 2, 2

ROWS = ((1, -1), (0, 0), (2, 1), (-1, 2))

ARRIVE = (('QR', 'QL'), ('FR', 'FL'), ('QM', 'ML', 'MR', 'MO'), ('S1', 'S2', 'S3', 'S4', 'S5'),
          ('HR0', 'HR1', 'HL0', 'HL1', 'MB', 'MC'), ('TR', 'TL'),
          ('MA', 'DR0', 'DR1', 'DL0', 'DL1', 'AR', 'AL'))
NEAR, FAR, QUERIES, LSE, HOPS, SUM_LSE, LAST = range(len(ARRIVE))
LEAVE = (('QR', 'QL', 'FR', 'FL', 'QM', 'ML', 'MR', 'MO'),
         ('HR0', 'HR1', 'HL0', 'HL1', 'MA', 'MB', 'MC', 'DR0', 'DR1', 'DL0', 'DL1', 'AR', 'AL'),
         ('S1', 'S2', 'S3', 'S4', 'S5', 'TR', 'TL'))
ARRIVE_SEM = {k: c for c, ks in enumerate(ARRIVE) for k in ks}
LEAVE_SEM = {k: c for c, ks in enumerate(LEAVE) for k in ks}


def kernel(n, len_hbm, q_hbm, c_hbm, out_v,
           len_ref, q_st, q_v, c_v, o_v, lse_c, z_own, z_mate, y_s, y_l, y_r, t_s, t_l, t_r, wrow, wt, m_a, m_b, m_c, h_p, h_n, d_p, d_n, a_p, a_n, r_p, r_n,
           send, recv, len_sem, q_sem, c_sem):
    G = q_v.shape[0]
    lat = o_v.shape[3]
    heads = o_v.shape[2]
    hl = heads // n
    sl = c_v.shape[3]
    nc = n // 2
    me = lax.axis_index('dcp')
    chip = lax.div(me, 2)
    core = lax.rem(me, 2)

    def dev(dx, other):
        return 2 * lax.rem(chip + dx + nc, nc) + (1 - core if other else core)

    def hd(d):
        return pl.ds(pl.multiple_of(d * hl, hl), hl)

    first, second, both = pl.ds(0, H), pl.ds(H, H), pl.ds(0, SC)
    pairs, pairs1, pairs2 = pl.ds(0, H), pl.ds(0, H // 2), pl.ds(H // 2, H // 2)
    right, left, opp, mate = dev(1, 0), dev(-1, 0), dev(2, 0), dev(0, 1)
    right1, left1, opp1 = dev(1, 1), dev(-1, 1), dev(2, 1)

    def same_q(g, part, d):
        r = q_v.at[g, part, hd(d)]
        return r, r

    def msg(kind, g):
        if kind == 'QR':
            src, dst = same_q(g, pairs, me)
            to = right
        elif kind == 'QL':
            src, dst = same_q(g, pairs, me)
            to = left
        elif kind == 'FR':
            src, dst = same_q(g, pairs1, left)
            to = right
        elif kind == 'FL':
            src, dst = same_q(g, pairs2, right)
            to = left
        elif kind == 'ML':
            src, dst = same_q(g, pairs, left)
            to = mate
        elif kind == 'MR':
            src, dst = same_q(g, pairs, right)
            to = mate
        elif kind == 'MO':
            src, dst = same_q(g, pairs, opp)
            to = mate
        elif kind == 'QM':
            src, dst = same_q(g, pairs, me)
            to = mate
        elif kind == 'TR':
            src, dst, to = t_s.at[g], t_l.at[g], right
        elif kind == 'TL':
            src, dst, to = t_s.at[g], t_r.at[g], left
        elif kind == 'S1':
            src, dst, to = z_own.at[g], z_mate.at[g], mate
        elif kind == 'S2':
            src, dst, to = y_s.at[0, g], y_l.at[0, g], right
        elif kind == 'S3':
            src, dst, to = y_s.at[0, g], y_l.at[1, g], right1
        elif kind == 'S4':
            src, dst, to = y_s.at[1, g], y_r.at[0, g], left
        elif kind == 'S5':
            src, dst, to = y_s.at[1, g], y_r.at[1, g], left1
        elif kind == 'MA':
            src, dst, to = o_v.at[g, both, hd(mate)], m_a.at[g], mate
        elif kind == 'MB':
            src, dst, to = o_v.at[g, first, hd(right1)], m_b.at[g], mate
        elif kind == 'MC':
            src, dst, to = o_v.at[g, second, hd(left1)], m_c.at[g], mate
        elif kind == 'HR0':
            src, dst, to = o_v.at[g, first, hd(opp)], h_p.at[0, g], right
        elif kind == 'HR1':
            src, dst, to = o_v.at[g, first, hd(opp1)], h_p.at[1, g], right1
        elif kind == 'HL0':
            src, dst, to = o_v.at[g, second, hd(opp)], h_n.at[0, g], left
        elif kind == 'HL1':
            src, dst, to = o_v.at[g, second, hd(opp1)], h_n.at[1, g], left1
        elif kind == 'DR0':
            src, dst, to = o_v.at[g, second, hd(right)], d_p.at[0, g], right
        elif kind == 'DR1':
            src, dst, to = o_v.at[g, second, hd(right1)], d_p.at[1, g], right1
        elif kind == 'DL0':
            src, dst, to = o_v.at[g, first, hd(left)], d_n.at[0, g], left
        elif kind == 'DL1':
            src, dst, to = o_v.at[g, first, hd(left1)], d_n.at[1, g], left1
        elif kind == 'AR':
            src, dst, to = a_p.at[g], r_p.at[g], right
        else:
            src, dst, to = a_n.at[g], r_n.at[g], left
        return pltpu.make_async_remote_copy(
            src_ref=src, dst_ref=dst, send_sem=send.at[LEAVE_SEM[kind]], recv_sem=recv.at[ARRIVE_SEM[kind], g],
            device_id={'dcp': to}, device_id_type=pl.DeviceIdType.MESH)

    def start(g, *kinds):
        for k in kinds:
            msg(k, g).start()

    arrive_bytes = (q_v.at[0, pairs, 0:2 * hl], q_v.at[0, pairs, 0:hl], q_v.at[0, pairs, 0:4 * hl], z_own.at[0:3],
                    o_v.at[0, 0:3, 0:4 * hl], z_own.at[0], o_v.at[0, both, 0:5 * hl])
    leave_bytes = (q_v.at[:, :, 0:7 * hl], o_v, lse_c.at[0, 0:8 * G])

    def pending(ref, g, c):
        return pltpu.make_async_remote_copy(
            src_ref=ref, dst_ref=ref, send_sem=send.at[c % len(LEAVE)], recv_sem=recv.at[c, g],
            device_id={'dcp': mate}, device_id_type=pl.DeviceIdType.MESH)

    def arrived(g, c):
        pending(arrive_bytes[c], g, c).wait_recv()

    def load(g):
        slot = lax.rem(g, 2)
        return pltpu.make_async_copy(c_hbm.at[g], c_v.at[slot], c_sem.at[slot])

    barrier = pltpu.get_barrier_semaphore()
    for d in (mate, right, right1, left, left1):
        pl.semaphore_signal(barrier, inc=1, device_id={'dcp': d}, device_id_type=pl.DeviceIdType.MESH)

    def fetch(k):
        part = pl.ds(0, 1) if k == 0 else pl.ds(1, G - 1)
        return pltpu.make_async_copy(q_hbm.at[part], q_st.at[part], q_sem.at[k])

    fetch(0).start()
    fetch(1).start()
    lens = pltpu.make_async_copy(len_hbm, len_ref, len_sem)
    lens.start()
    for g in range(min(2, G)):
        load(g).start()
    wrow[...] = jnp.zeros_like(wrow)

    def pack(g):
        for p in range(H):
            a, b = q_st[g, 2 * p], q_st[g, 2 * p + 1]
            q_v[g, p, hd(me), :lat] = a[:, :lat]
            q_v[g, p, hd(me), lat:2 * lat] = b[:, :lat]
            q_v[g, p, hd(me), 2 * lat:] = jnp.concatenate([a[:, lat:], b[:, lat:]], axis=1)

    for g in range(min(QD, G)):
        if g < 2:
            fetch(g).wait()
        pack(g)
        if g == 0:
            pl.semaphore_wait(barrier, 5)
        start(g, 'QR', 'QL', 'QM')
    lens.wait()

    def attention(g):
        load(g).wait()
        pos = me * sl + lax.broadcasted_iota(jnp.int32, (1, sl), 1)

        def scores(i):
            c = c_v.at[lax.rem(g, 2), i]
            p, r = divmod(i, 2)
            rope = q_v[g, p, :, 2 * lat + r * ROPE:2 * lat + (r + 1) * ROPE]
            return (jnp.dot(q_v[g, p, :, r * lat:(r + 1) * lat], c[:lat], preferred_element_type=F32)
                    + jnp.dot(rope, c[lat:], preferred_element_type=F32))

        ahead = scores(0)
        for i in range(SC):
            c = c_v.at[lax.rem(g, 2), i]
            s, ahead = ahead, scores(i + 1) if i + 1 < SC else None
            s = jnp.where(pos < len_ref[g * SC + i], s * SCALE, -jnp.inf)
            m = jnp.max(s, axis=1, keepdims=True)
            m0 = jnp.where(m > -jnp.inf, m, 0.0)
            p = jnp.exp(s - m0)
            l = jnp.sum(p, axis=1, keepdims=True)
            pv = lax.dot_general(p.astype(BF16), c[:lat], NT, preferred_element_type=F32)
            has = l > 0.0
            l1 = jnp.where(has, l, 1.0)
            o_v[g, i] = (pv * (1.0 / l1)).astype(BF16)
            lse_c[i] = jnp.broadcast_to(jnp.where(has, m0 + jnp.log(l1), -jnp.inf), (heads, 128))
        lane = lax.broadcasted_iota(jnp.int32, (2 * hl, 128), 1)
        columns = []
        for i in range(SC):
            block = jnp.zeros((2 * hl, 128), F32)
            for r, steps in enumerate(ROWS):
                c = lax.rem(chip + steps[i // H] + nc, nc)
                block = jnp.where(lane == r, lse_c[i, pl.ds(pl.multiple_of(c * 2 * hl, 2 * hl), 2 * hl)], block)
            columns.append(block)
        rows = jnp.concatenate(columns, axis=0).T
        z_own[g] = rows[:2]
        y_s[0, g] = rows[2:3]
        y_s[1, g] = rows[3:4]

    early = lax.broadcasted_iota(jnp.int32, (1, 128), 1) < 2 * hl * H

    def softmax(ls):
        mx = functools.reduce(jnp.maximum, ls)
        mx = jnp.where(mx > -jnp.inf, mx, 0.0)
        es = [jnp.exp(x - mx) for x in ls]
        z = functools.reduce(jnp.add, es)
        has = z > 0.0
        z1 = jnp.where(has, z, 1.0)
        r = 1.0 / z1
        for k, e in enumerate(es):
            wrow[k:k + 1, :] = e * r
        wt[...] = wrow[...].T
        return jnp.where(has, mx + jnp.log(z1), -jnp.inf)

    def weighted(k, i, o):
        w = wt[pl.ds(pl.multiple_of((2 * i + core) * hl, hl), hl)]
        return w[:, k:k + 1] * o.astype(F32)

    def sums(g):
        arrived(g, LSE)
        t_s[g] = softmax([z_own[g, 0:1], z_mate[g, 0:1]] + [jnp.where(early, y_l[k, g], y_r[k, g]) for k in range(2)])
        start(g, 'TR', 'TL')
        arrived(g, HOPS)
        for i0, d, m, h, a, k in ((0, right, m_b, h_p, a_p, 'AR'), (H, left, m_c, h_n, a_n, 'AL')):
            for j in range(H):
                i = i0 + j
                a[g, j] = (weighted(0, i, o_v[g, i, hd(d)]) + weighted(1, i, m[g, j])
                           + weighted(2, i, h[0, g, j]) + weighted(3, i, h[1, g, j]))
            start(g, k)

    def final(g):
        arrived(g, SUM_LSE)
        softmax([z_own[g, 1:2], z_mate[g, 1:2]] + [jnp.where(early, y_r[k, g], y_l[k, g]) for k in range(2)]
                + [jnp.where(early, t_l[g], t_r[g])])
        arrived(g, LAST)
        for i in range(SC):
            d, r, j = (d_n, r_p, i) if i < H else (d_p, r_n, i - H)
            out_v[g, i] = (weighted(0, i, o_v[g, i, hd(me)]) + weighted(1, i, m_a[g, i])
                           + weighted(2, i, d[0, g, j]) + weighted(3, i, d[1, g, j])
                           + weighted(4, i, r[g, j])).astype(BF16)

    def stage(t, lag, extra=0):
        g = t - lag
        return g, (g >= 0) & (g < G - extra)

    def step(t, carry):
        a, on = stage(t, 0)

        @pl.when(on)
        def _():
            arrived(a, NEAR)
            start(a, 'FR', 'FL', 'ML', 'MR')

        for h in range(QD, G):
            @pl.when(t == OWN_AT.get(h, h - QD))
            def _():
                pack(h)
                start(h, 'QR', 'QL', 'QM')

        b, on = stage(t, 1)
        on = on & (t != 2)

        @pl.when(on)
        def _():
            arrived(b, FAR)
            start(b, 'MO')

        e, on = stage(t, 2 + D2)

        @pl.when(on)
        def _():
            start(e, 'DR0', 'DR1', 'DL0', 'DL1')

        g, on = stage(t, 2)

        @pl.when(on)
        def _():
            arrived(g, QUERIES)
            attention(g)
            start(g, 'HR0', 'HR1', 'HL0', 'HL1', 'S1', 'S2', 'S3', 'S4', 'S5', 'MB', 'MC', 'MA')

        b, on = stage(t, 1)
        on = on & (t == 2)

        @pl.when(on)
        def _():
            arrived(b, FAR)
            start(b, 'MO')

        @pl.when(stage(t, 2, 2)[1])
        def _():
            load(t).start()

        d, on = stage(t, 2 + D1)

        @pl.when(on)
        def _():
            sums(d)

        return carry

    lax.fori_loop(0, G + 2, step, 0)

    def direct(g, carry):
        start(g, 'DR0', 'DR1', 'DL0', 'DL1')
        return carry

    lax.fori_loop(G - D2, G, direct, 0)

    def rest(g, carry):
        sums(g)
        return carry

    lax.fori_loop(G - D1, G, rest, 0)

    def finish(g, carry):
        final(g)
        return carry

    lax.fori_loop(0, G, finish, 0)
    for c, ref in enumerate(leave_bytes):
        pending(ref, 0, c).wait_send()


def solution(mesh):
    n = mesh.shape['dcp']

    def local(q, cache, lengths):
        b, sl, wd = cache.shape
        hl = q.shape[1]
        heads = hl * n
        lat = wd - ROPE
        G = b // SC
        ct = jnp.swapaxes(cache, 1, 2).reshape(G, SC, wd, sl)
        vmem = pltpu.VMEM
        out = pl.pallas_call(
            functools.partial(kernel, n),
            out_shape=vmem((G, SC, hl, lat), BF16),
            in_specs=[pl.BlockSpec(memory_space=pl.ANY)] * 3,
            out_specs=pl.BlockSpec(memory_space=pltpu.VMEM),
            scratch_shapes=[
                pltpu.SMEM((b,), jnp.int32),
                vmem((G, SC, hl, wd), BF16),
                vmem((G, H, heads, 2 * wd), BF16),
                vmem((2, SC, wd, sl), BF16),
                vmem((G, SC, heads, lat), BF16),
                vmem((SC, heads, 128), F32),
                vmem((G, 2, 128), F32),
                vmem((G, 2, 128), F32),
                vmem((2, G, 1, 128), F32),
                vmem((2, G, 1, 128), F32),
                vmem((2, G, 1, 128), F32),
                vmem((G, 1, 128), F32),
                vmem((G, 1, 128), F32),
                vmem((G, 1, 128), F32),
                vmem((128, 128), F32),
                vmem((128, 128), F32),
                vmem((G, SC, hl, lat), BF16),
                vmem((G, H, hl, lat), BF16),
                vmem((G, H, hl, lat), BF16),
                vmem((2, G, H, hl, lat), BF16),
                vmem((2, G, H, hl, lat), BF16),
                vmem((2, G, H, hl, lat), BF16),
                vmem((2, G, H, hl, lat), BF16),
                vmem((G, H, hl, lat), F32),
                vmem((G, H, hl, lat), F32),
                vmem((G, H, hl, lat), F32),
                vmem((G, H, hl, lat), F32),
                pltpu.SemaphoreType.DMA((len(LEAVE),)),
                pltpu.SemaphoreType.DMA((len(ARRIVE), G)),
                pltpu.SemaphoreType.DMA,
                pltpu.SemaphoreType.DMA((2,)),
                pltpu.SemaphoreType.DMA((2,)),
            ],
            compiler_params=pltpu.CompilerParams(
                collective_id=0, has_side_effects=True, vmem_limit_bytes=56 * 2 ** 20),
        )(lengths, q.reshape(G, SC, hl, wd), ct)
        return out.reshape(b, hl, lat)

    return jax.shard_map(local, mesh=mesh, in_specs=(P('dp', 'dcp', None), P('dp', 'dcp', None), P('dp')),
                         out_specs=P('dp', 'dcp', None), check_vma=False)
```
